256 devices in a mesh: pipe: 8 (over x, z_lo), tensor: 4 (over y), expert: 8 (over z_hi, core).
Axes of the slice: x: 4, y: 4, z: 8 (z_hi: 4, z_lo: 2; z = z_hi * 2 + z_lo), core: 2. Of those that a mesh axis runs over, the one named last changes fastest.
Arguments:
- tokens: bfloat16 [2, 512, 4096], P(None, 'expert'), may hold values from -6 to 6
- gains: float32 [8, 4096], P('pipe'), may hold values from 0.1 to 1.9
- route_ids: int32 [8, 2, 512, 2], P('pipe', None, 'expert'), may hold values from 0 to 7, all different within a row
- route_weights: float32 [8, 2, 512, 2], P('pipe', None, 'expert'), may hold values from 0.2 to 1
- picks: int32 [8, 2, 8, 64], P('pipe', None, 'expert'), may hold values from 0 to 63, each once within a row
- w_gate: bfloat16 [8, 8, 4096, 1536], P('pipe', 'expert', None, 'tensor'), may hold values from -0.09375 to 0.09375
- w_up: bfloat16 [8, 8, 4096, 1536], P('pipe', 'expert', None, 'tensor'), may hold values from -0.09375 to 0.09375
- w_down: bfloat16 [8, 8, 1536, 4096], P('pipe', 'expert', 'tensor'), may hold values from -0.15625 to 0.15625
Outputs:
- streams: bfloat16 [8, 2, 512, 4096], P('pipe', None, 'expert', 'tensor')
The draws below stay inside these ranges and needn't reach their ends.
Inputs may be any that keep to these rules, and one draw needn't show every extreme that they name: `route_ids`: each token names 2 different experts; every expert is named by some token. `picks`: for every layer, micro-batch and block of 64 tokens, a permutation of 0 to 63.
All inputs are finite; a program needn't handle non-finite values.
Results may differ from the reference program's by a relative error of at most 0.025.
Values may be sent and summed in bfloat16 or wider, within the bound.
A program may use at most 64 MiB of HBM per device.

```python
import jax
import jax.numpy as jnp
from jax import lax

D = 4096
FF = 1536
TOPK = 2
MICRO = 2
TOK_DEV = 64
EXPERTS = 8
QUARTER = 16
CAP = 5
TOKENS = 512
N_PIPE = 8
N_TENSOR = 4
N_EXPERT = 8


def steps_of(rng, shape, shards, low, top_value):
    loudness, own = 1.0, jax.random.fold_in(rng, 6)
    for dim, parts in shards:
        steps = jnp.exp(jax.random.uniform(jax.random.fold_in(own, dim), (parts,), jnp.float32, low / len(shards), top_value / len(shards)))
        loudness = loudness * jnp.repeat(steps, shape[dim] // parts).reshape([-1 if axis == dim else 1 for axis in range(len(shape))])
    return loudness


def different_ones(stream_key, rows, number_of, top, lift):
    sequence = jax.random.permutation(jax.random.fold_in(stream_key, 1), number_of)
    pull = sequence
    for power in range(3):
        pull = pull * pull // number_of
    pull = pull * lift // number_of
    lots = jax.random.randint(jax.random.fold_in(stream_key, 2), (rows, number_of), 0, 4096) + pull
    fixed_rows = jax.random.permutation(jax.random.fold_in(stream_key, 3), rows)[jnp.arange(number_of) % rows]
    lots = jnp.where(jnp.arange(rows)[:, None] == fixed_rows[None, :], 1 << 14, lots)
    priority = lots * number_of + jnp.arange(number_of)
    return lax.top_k(priority.astype(jnp.int32), top)[1].astype(jnp.int32)


def gaussian(key, shape, deviation, most, pieces=(), kind=jnp.bfloat16):
    values = jax.random.normal(key, shape, jnp.float32) * deviation
    if len(pieces) > 0:
        values = steps_of(key, shape, pieces, -0.22, 0.18) * values
    return jnp.clip(values, min=-most, max=most).astype(kind)


def setup_inputs(seed: int = 0) -> dict:
    key_list = jax.random.split(jax.random.key(seed), 9)
    tokens = gaussian(key_list[0], (MICRO, TOKENS, D), 1.0, 6.0, ((1, 8),))
    gains = jnp.clip(1.0 + 0.18 * jax.random.normal(key_list[1], (N_PIPE, D), jnp.float32), 0.1, 1.9)
    route_ids = different_ones(key_list[2], N_PIPE * MICRO * TOKENS, EXPERTS, TOPK, 4096).reshape((N_PIPE, MICRO, TOKENS, TOPK))
    route_weights = jnp.clip(0.2 + 0.8 * jax.random.uniform(key_list[3], (N_PIPE, MICRO, TOKENS, TOPK), jnp.float32) ** steps_of(key_list[3], (N_PIPE, MICRO, TOKENS, TOPK), ((0, 8), (2, 8)), -0.2, 0.2), 0.2, 1.0)
    picks = jax.vmap(lambda own: jax.random.permutation(own, TOK_DEV))(jax.random.split(key_list[4], N_PIPE * MICRO * N_EXPERT)).reshape((N_PIPE, MICRO, N_EXPERT, TOK_DEV)).astype(jnp.int32)
    w_gate = gaussian(key_list[5], (N_PIPE, EXPERTS, D, FF), D ** -0.5, 0.09375, ((0, 8), (1, 8), (3, 4)))
    w_up = gaussian(key_list[6], (N_PIPE, EXPERTS, D, FF), D ** -0.5, 0.09375, ((0, 8), (1, 8), (3, 4)))
    w_down = gaussian(key_list[7], (N_PIPE, EXPERTS, FF, D), FF ** -0.5, 0.15625, ((0, 8), (1, 8), (2, 4)))
    return dict(tokens=tokens, gains=gains, route_ids=route_ids, route_weights=route_weights, picks=picks, w_gate=w_gate, w_up=w_up, w_down=w_down)


epsilon = 1e-06

def find_slots(ordered_ids, capacity):
    onehot = (ordered_ids[..., None] == jnp.arange(EXPERTS, dtype=jnp.int32)).astype(jnp.int32)
    earlier = jnp.cumsum(onehot, axis=-2) - onehot
    slot_index = lax.optimization_barrier(jnp.sum(earlier * onehot, axis=-1))
    return (slot_index, slot_index < capacity)

def expert_ffn(operands):
    row_block, gate_matrix, up_matrix, down_matrix = operands
    gate_val = jnp.dot(row_block, gate_matrix, preferred_element_type=jnp.float32)
    up_val = jnp.dot(row_block, up_matrix, preferred_element_type=jnp.float32)
    hidden = (jax.nn.silu(gate_val) * up_val).astype(jnp.bfloat16)
    shard_width = FF // N_TENSOR
    summed = jnp.zeros((row_block.shape[0], D), jnp.float32)
    for shard_index in range(N_TENSOR):
        lower = shard_index * shard_width
        partial_sum = jnp.dot(hidden[:, lower:lower + shard_width], down_matrix[lower:lower + shard_width], preferred_element_type=jnp.float32)
        rounded = lax.optimization_barrier(partial_sum.astype(jnp.bfloat16))
        summed = summed + rounded.astype(jnp.float32)
    return summed.astype(jnp.bfloat16)

def moe_section(stream, gain_row, section_ids, section_weights, section_picks, gate_all, up_all, down_all):
    groups = N_EXPERT
    offsets = (jnp.arange(groups, dtype=jnp.int32) * TOK_DEV)[:, None]
    ordered = (section_picks + offsets).astype(jnp.int32).reshape(groups, N_TENSOR, QUARTER)
    stream_f = stream.astype(jnp.float32)
    inv_rms = lax.rsqrt(lax.optimization_barrier(jnp.mean(stream_f * stream_f, axis=1, keepdims=True)) + epsilon)
    normed = (stream_f * inv_rms * gain_row[None, :]).astype(jnp.bfloat16)
    ordered_ids = section_ids[ordered].reshape(groups, N_TENSOR, QUARTER * TOPK)
    ordered_weights = section_weights[ordered].reshape(groups, N_TENSOR, QUARTER * TOPK)
    slot_index, kept_mask = find_slots(ordered_ids, CAP)
    route_tokens = jnp.repeat(ordered, TOPK, axis=2)
    group_index = jnp.arange(groups, dtype=jnp.int32)[:, None, None]
    rank_index = jnp.arange(N_TENSOR, dtype=jnp.int32)[None, :, None]
    position = ((ordered_ids * groups + group_index) * N_TENSOR + rank_index) * CAP + slot_index
    filled = EXPERTS * groups * N_TENSOR * CAP
    target = jnp.where(kept_mask, position, filled).astype(jnp.int32)
    source = jnp.full((filled + 1,), TOKENS, jnp.int32).at[target.reshape(-1)].set(route_tokens.reshape(-1))
    padded = jnp.concatenate([normed, jnp.zeros((1, D), jnp.bfloat16)], axis=0)
    row_block = padded[source[:filled]].reshape(EXPERTS, groups * N_TENSOR * CAP, D)
    results = lax.map(expert_ffn, (row_block, gate_all, up_all, down_all))
    flat_results = jnp.concatenate([results.reshape(filled, D), jnp.zeros((1, D), jnp.bfloat16)], axis=0)
    picked = flat_results[target].astype(jnp.float32)
    weighted = picked * (ordered_weights * kept_mask)[..., None]
    update = lax.optimization_barrier(jnp.sum(weighted.reshape(groups, N_TENSOR, QUARTER, TOPK, D), axis=3))
    stream_new = stream_f.at[ordered.reshape(-1)].add(update.reshape(-1, D))
    return stream_new.astype(jnp.bfloat16)

def reference(tokens, gains, route_ids, route_weights, picks, w_gate, w_up, w_down):
    finished = []
    for micro_index in range(MICRO):
        stream = tokens[micro_index]
        column = []
        for section_index in range(N_PIPE):
            stream = moe_section(stream, gains[section_index], route_ids[section_index, micro_index], route_weights[section_index, micro_index], picks[section_index, micro_index], w_gate[section_index], w_up[section_index], w_down[section_index])
            column.append(stream)
        finished.append(jnp.stack(column))
    return jnp.stack(finished, axis=1)
```

```python
import jax
import jax.numpy as jnp
from jax import lax
from jax.experimental import pallas as pl
from jax.experimental.pallas import tpu as pltpu
from jax.sharding import PartitionSpec as P

EPS = 1e-06
MESH = pl.DeviceIdType.MESH
BF = jnp.bfloat16
F32 = jnp.float32
CHUNKS = 4
CAP = 5


def wait_bytes(ref, sem):
    pltpu.make_async_copy(ref, ref, sem).wait()


def relay_kernel(
    tokens, gains, rt_own, rt_next, rt_col, w_gate, w_up, w_down, out,
    wgu, wd, place, comb, hin, hnew, xs, dfirst, dout, opp, side, relay, got, rout, ret, outbuf,
    wsem, hsem, dsem, agsem, rssem, retsem, osem, fsem,
    s_tok, s_disp, s_ag, s_rs, s_ret, s_h, s_out,
):
    sec = lax.axis_index("pipe")
    rank = lax.axis_index("tensor")
    me = lax.axis_index("expert")
    last = lax.axis_size("pipe") - 1
    up1 = lax.rem(rank + 1, 4)
    dn1 = lax.rem(rank + 3, 4)
    far = lax.rem(rank + 2, 4)

    def send(src, dst, ssem, rsem, dev):
        pltpu.make_async_remote_copy(
            src_ref=src, dst_ref=dst, send_sem=ssem, recv_sem=rsem,
            device_id=dev, device_id_type=MESH,
        ).start()

    barrier = pltpu.get_barrier_semaphore()

    def greet(dev):
        pl.semaphore_signal(barrier, inc=1, device_id=dev, device_id_type=MESH)

    for o in range(1, 8):
        greet({"expert": lax.rem(me + o, 8)})
    greet({"tensor": up1})
    greet({"tensor": dn1})

    @pl.when(sec < last)
    def _():
        for e in range(8):
            greet({"pipe": sec + 1, "expert": e})

    @pl.when(sec > 0)
    def _():
        for e in range(8):
            greet({"pipe": sec - 1, "expert": e})

    def weight_copies():
        copies = []
        for q in range(4):
            copies.append((w_gate.at[pl.ds(q * 1024, 1024), :], wgu.at[q, :, pl.ds(0, 384)]))
            copies.append((w_up.at[pl.ds(q * 1024, 1024), :], wgu.at[q, :, pl.ds(384, 384)]))
        for q in range(4):
            copies.append((w_down.at[:, pl.ds(q * 1024, 1024)], wd.at[q]))
        return [pltpu.make_async_copy(a, b, wsem.at[i]) for i, (a, b) in enumerate(copies)]

    for copy in weight_copies():
        copy.start()

    slot_rows = lax.broadcasted_iota(jnp.int32, (640, 256), 0).astype(F32)
    slot_cols = lax.broadcasted_iota(jnp.int32, (256, 640), 1).astype(F32)

    def placing(rt, k):
        t = rt[k]
        hit = (slot_rows == t[0:1, :]) | (slot_rows == t[1:2, :])
        return jnp.where(hit, 1.0, 0.0).astype(BF)

    def build(k, carry):
        place[k] = placing(rt_next, k)
        c = rt_col[k]
        mix = jnp.where(slot_cols == c[:, 0:1], c[:, 2:3], 0.0)
        mix = mix + jnp.where(slot_cols == c[:, 1:2], c[:, 3:4], 0.0)
        high = mix.astype(BF)
        comb[k, 0] = high
        comb[k, 1] = (mix - high.astype(F32)).astype(BF)
        return carry

    lax.fori_loop(0, CHUNKS, build, 0)

    greeted = 9 + jnp.where(sec < last, 8, 0) + jnp.where(sec > 0, 8, 0)
    pl.semaphore_wait(barrier, greeted)

    def place_rows(matrix, rows, dest, k):
        moved = jnp.dot(matrix, rows, preferred_element_type=F32).astype(BF)
        for e in range(8):
            dest[k, e] = moved[e * 80 : (e + 1) * 80]

    my_half = me // 4

    @pl.when(sec == 0)
    def _():
        lane = pl.multiple_of(rank * 1024, 128)
        row = pl.multiple_of(lax.rem(me, 4) * 64, 64)
        for m in range(2):
            k = m * 2 + my_half
            for o in range(1, 8):
                j = lax.rem(me + o, 8)
                send(
                    tokens.at[m, :, pl.ds(pl.multiple_of(lane + j * 128, 128), 128)],
                    hin.at[k, pl.ds(row, 64), :],
                    s_tok.at[m, o - 1], hsem.at[k], {"expert": j},
                )
            pltpu.make_async_copy(
                tokens.at[m, :, pl.ds(pl.multiple_of(lane + me * 128, 128), 128)],
                hin.at[k, pl.ds(row, 64), :], hsem.at[k],
            ).start()

        def first(k, carry):
            wait_bytes(hin.at[k], hsem.at[k])
            place_rows(placing(rt_own, k), hin[k], dfirst, k)
            for o in range(1, 8):
                e = lax.rem(me + o, 8)
                send(dfirst.at[k, e], xs.at[k, 0, me], fsem.at[k], dsem.at[k, my_half], {"expert": e})
            pltpu.make_async_copy(dfirst.at[k, me], xs.at[k, 0, me], dsem.at[k, my_half]).start()
            return carry

        lax.fori_loop(0, CHUNKS, first, 0)

    for copy in weight_copies():
        copy.wait()

    lo, hi = pl.ds(0, 4), pl.ds(4, 4)
    to_up, to_dn = {"tensor": up1}, {"tensor": dn1}

    def rows_of(k, rel):
        return jnp.concatenate([xs[k, rel, j] for j in range(8)], axis=1)

    def step(k, carry):
        ssem = s_ag.at[k]
        wait_bytes(xs.at[k, 0, lo], dsem.at[k, 0])
        send(xs.at[k, 0, lo], xs.at[k, 1, lo], ssem, agsem.at[k, 0], to_up)
        wait_bytes(xs.at[k, 0, hi], dsem.at[k, 1])
        send(xs.at[k, 0, hi], xs.at[k, 2, hi], ssem, agsem.at[k, 1], to_dn)
        send(xs.at[k, 0, lo], xs.at[k, 2, lo], ssem, agsem.at[k, 2], to_dn)
        send(xs.at[k, 0, hi], xs.at[k, 1, hi], ssem, agsem.at[k, 3], to_up)

        def part(rel, origin):
            x = rows_of(k, rel).astype(F32)
            squares = jnp.sum(x * x, axis=1, keepdims=True)
            scaled = (x * gains[pl.ds(origin, 1), :]).astype(BF)
            return squares, jnp.dot(scaled, wgu[origin], preferred_element_type=F32)

        squares, both = part(0, rank)
        wait_bytes(xs.at[k, 1, lo], agsem.at[k, 0])
        send(xs.at[k, 1, lo], xs.at[k, 3, lo], ssem, agsem.at[k, 4], to_up)
        wait_bytes(xs.at[k, 2, hi], agsem.at[k, 1])
        send(xs.at[k, 2, hi], xs.at[k, 3, hi], ssem, agsem.at[k, 5], to_dn)
        wait_bytes(xs.at[k, 1, hi], agsem.at[k, 3])
        sq, b = part(1, dn1)
        squares, both = squares + sq, both + b
        wait_bytes(xs.at[k, 2, lo], agsem.at[k, 2])
        sq, b = part(2, up1)
        squares, both = squares + sq, both + b
        wait_bytes(xs.at[k, 3, lo], agsem.at[k, 4])
        wait_bytes(xs.at[k, 3, hi], agsem.at[k, 5])
        sq, b = part(3, far)
        squares, both = squares + sq, both + b
        both = both * lax.rsqrt(squares * (1.0 / 4096.0) + EPS)
        gate, up = both[:, :384], both[:, 384:]
        hidden = (gate / (1.0 + jnp.exp(-gate)) * up).astype(BF)

        def down(q):
            return jnp.dot(hidden, wd[q], preferred_element_type=F32)

        def lanes(value, j):
            return value[:, j * 128 : (j + 1) * 128]

        ssem = s_rs.at[k]
        value = down(far)
        for j in range(8):
            opp[k, j] = lanes(value, j).astype(BF)
        send(opp.at[k, lo], relay.at[k, 0], ssem, rssem.at[k, 0], to_up)
        send(opp.at[k, hi], relay.at[k, 1], ssem, rssem.at[k, 1], to_dn)
        above = down(up1)
        for j in range(4, 8):
            side[k, 0, j] = lanes(above, j).astype(BF)
        send(side.at[k, 0, hi], got.at[k, 0, hi], ssem, rssem.at[k, 2], to_up)
        below = down(dn1)
        for j in range(4):
            side[k, 1, j] = lanes(below, j).astype(BF)
        send(side.at[k, 1, lo], got.at[k, 1, lo], ssem, rssem.at[k, 3], to_dn)
        wait_bytes(relay.at[k, 0], rssem.at[k, 0])
        for j in range(4):
            side[k, 0, j] = (lanes(above, j) + relay[k, 0, j].astype(F32)).astype(BF)
        send(side.at[k, 0, lo], got.at[k, 0, lo], ssem, rssem.at[k, 4], to_up)
        wait_bytes(relay.at[k, 1], rssem.at[k, 1])
        for j in range(4, 8):
            side[k, 1, j] = (lanes(below, j) + relay[k, 1, j - 4].astype(F32)).astype(BF)
        send(side.at[k, 1, hi], got.at[k, 1, hi], ssem, rssem.at[k, 5], to_dn)
        own = down(rank)

        def give_back(j):
            total = lanes(own, j) + got[k, 0, j].astype(F32) + got[k, 1, j].astype(F32)
            rout[k, j] = total.astype(BF)

        def ship(j):
            @pl.when(me == j)
            def _():
                pltpu.make_async_copy(rout.at[k, j], ret.at[k, me], retsem.at[k]).start()

            @pl.when(me != j)
            def _():
                send(rout.at[k, j], ret.at[k, me], s_ret.at[k], retsem.at[k], {"expert": j})

        wait_bytes(got.at[k, 1, lo], rssem.at[k, 3])
        wait_bytes(got.at[k, 0, lo], rssem.at[k, 4])
        for j in range(4):
            give_back(j)
        for j in range(4):
            ship(j)
        wait_bytes(got.at[k, 0, hi], rssem.at[k, 2])
        wait_bytes(got.at[k, 1, hi], rssem.at[k, 5])
        for j in range(4, 8):
            give_back(j)
        for j in range(4, 8):
            ship(j)

        @pl.when(sec > 0)
        def _():
            wait_bytes(hin.at[k], hsem.at[k])

        wait_bytes(ret.at[k], retsem.at[k])
        back = ret[k].reshape(640, 128)
        update = jnp.dot(comb[k, 0], back, preferred_element_type=F32)
        update = update + jnp.dot(comb[k, 1], back, preferred_element_type=F32)
        fresh = (hin[k].astype(F32) + update).astype(BF)
        hnew[k] = fresh

        @pl.when(sec < last)
        def _():
            place_rows(place[k], fresh, dout, k)
            for e in range(8):
                send(
                    dout.at[k, e], xs.at[k, 0, me], s_disp.at[k], dsem.at[k, my_half],
                    {"pipe": sec + 1, "expert": e},
                )
            send(hnew.at[k], hin.at[k], s_h.at[k], hsem.at[k], {"pipe": sec + 1})

        m, half = k // 2, lax.rem(k, 2)
        mine = pl.ds(pl.multiple_of(me * 128, 128), 128)
        for i in range(4):
            owner = half * 4 + i
            block = hnew.at[k, pl.ds(i * 64, 64), :]
            place_at = outbuf.at[m, :, mine]

            @pl.when(owner == me)
            def _():
                pltpu.make_async_copy(block, place_at, osem).start()

            @pl.when(owner != me)
            def _():
                send(block, place_at, s_out.at[k, i], osem, {"expert": owner})

        return carry

    lax.fori_loop(0, CHUNKS, step, 0)

    @pl.when(sec == 0)
    def _():
        for m in range(2):
            for o in range(7):
                wait_bytes(hin.at[m, pl.ds(0, 64), :], s_tok.at[m, o])
        for k in range(CHUNKS):
            wait_bytes(dfirst.at[k, pl.ds(0, 7)], fsem.at[k])

    def drain(k, carry):
        wait_bytes(xs.at[k, pl.ds(0, 3)], s_ag.at[k])
        wait_bytes(xs.at[k, pl.ds(0, 3)], s_rs.at[k])
        wait_bytes(ret.at[k, pl.ds(0, 7)], s_ret.at[k])

        @pl.when(sec < last)
        def _():
            wait_bytes(dout.at[k], s_disp.at[k])
            wait_bytes(hnew.at[k], s_h.at[k])

        for i in range(4):
            owner = lax.rem(k, 2) * 4 + i

            @pl.when(owner != me)
            def _():
                wait_bytes(hnew.at[k, pl.ds(i * 64, 64), :], s_out.at[k, i])

        return carry

    lax.fori_loop(0, CHUNKS, drain, 0)
    wait_bytes(outbuf, osem)
    final = pltpu.make_async_copy(outbuf, out, wsem.at[0])
    final.start()
    final.wait()


def routing(route_ids, route_weights, picks):
    micro, tokens, routes = route_ids.shape
    group = lax.axis_index("expert")
    spot = jnp.arange(tokens, dtype=jnp.int32)
    place = jnp.sum(
        jnp.where(picks[:, :, None] == spot[None, None, :], spot[None, :, None], 0), axis=1
    )
    order = (place[:, :, None] * routes + jnp.arange(routes, dtype=jnp.int32)).reshape(micro, -1)
    quarter = order // (16 * routes)
    ids = route_ids.reshape(micro, -1)
    same = (ids[:, :, None] == ids[:, None, :]) & (quarter[:, :, None] == quarter[:, None, :])
    earlier = same & (order[:, None, :] < order[:, :, None])
    slot = jnp.sum(earlier.astype(jnp.int32), axis=2)
    row = ids * 80 + lax.rem(group, 4) * 20 + quarter * CAP + slot
    row = jnp.where(slot < CAP, row, -1).astype(F32).reshape(micro, tokens, routes)
    return jnp.concatenate(
        [jnp.swapaxes(row, 1, 2), jnp.swapaxes(route_weights, 1, 2)], axis=1
    )


def local(tokens, gains, route_ids, route_weights, picks, w_gate, w_up, w_down):
    mine = routing(route_ids[0], route_weights[0], picks[0, :, 0])
    sections = lax.axis_size("pipe")
    after = lax.ppermute(mine, "pipe", [(i + 1, i) for i in range(sections - 1)])
    every = lax.all_gather(jnp.stack([mine, after]), "expert")
    table = every.reshape(2, 4, 2, 2, 4, 64).transpose(2, 3, 0, 4, 1, 5).reshape(2, 4, 4, 256)
    columns = jnp.swapaxes(table[0], 1, 2)
    vmem = pl.BlockSpec(memory_space=pltpu.VMEM)
    anywhere = pl.BlockSpec(memory_space=pl.ANY)
    dma = pltpu.SemaphoreType.DMA
    out = pl.pallas_call(
        relay_kernel,
        name="relay",
        out_shape=jax.ShapeDtypeStruct((2, 64, 1024), BF),
        in_specs=[anywhere, vmem, vmem, vmem, vmem, anywhere, anywhere, anywhere],
        out_specs=anywhere,
        scratch_shapes=[
            pltpu.VMEM((4, 1024, 768), BF),
            pltpu.VMEM((4, 384, 1024), BF),
            pltpu.VMEM((CHUNKS, 640, 256), BF),
            pltpu.VMEM((CHUNKS, 2, 256, 640), BF),
            pltpu.VMEM((CHUNKS, 256, 128), BF),
            pltpu.VMEM((CHUNKS, 256, 128), BF),
            pltpu.VMEM((CHUNKS, 4, 8, 80, 128), BF),
            pltpu.VMEM((CHUNKS, 8, 80, 128), BF),
            pltpu.VMEM((CHUNKS, 8, 80, 128), BF),
            pltpu.VMEM((CHUNKS, 8, 80, 128), BF),
            pltpu.VMEM((CHUNKS, 2, 8, 80, 128), BF),
            pltpu.VMEM((CHUNKS, 2, 4, 80, 128), BF),
            pltpu.VMEM((CHUNKS, 2, 8, 80, 128), BF),
            pltpu.VMEM((CHUNKS, 8, 80, 128), BF),
            pltpu.VMEM((CHUNKS, 8, 80, 128), BF),
            pltpu.VMEM((2, 64, 1024), BF),
            dma((12,)),
            dma((CHUNKS,)),
            dma((CHUNKS, 2)),
            dma((CHUNKS, 6)),
            dma((CHUNKS, 6)),
            dma((CHUNKS,)),
            dma(()),
            dma((CHUNKS,)),
            dma((2, 7)),
            dma((CHUNKS,)),
            dma((CHUNKS,)),
            dma((CHUNKS,)),
            dma((CHUNKS,)),
            dma((CHUNKS,)),
            dma((CHUNKS, 4)),
        ],
        compiler_params=pltpu.CompilerParams(
            collective_id=0, has_side_effects=True, vmem_limit_bytes=56 * 1024 * 1024
        ),
    )(
        tokens, gains.reshape(4, 1024), table[0], table[1], columns,
        w_gate[0, 0], w_up[0, 0], w_down[0, 0],
    )
    return out[None]


def solution(mesh):
    return jax.shard_map(
        local,
        mesh=mesh,
        in_specs=(
            P(None, "expert", None),
            P("pipe", None),
            P("pipe", None, "expert", None),
            P("pipe", None, "expert", None),
            P("pipe", None, "expert", None),
            P("pipe", "expert", None, "tensor"),
            P("pipe", "expert", None, "tensor"),
            P("pipe", "expert", "tensor", None),
        ),
        out_specs=P("pipe", None, "expert", "tensor"),
        check_vma=False,
    )
```

```python
import jax
import jax.numpy as jnp
from jax import lax
from jax.experimental import pallas as pl
from jax.experimental.pallas import tpu as pltpu
from jax.sharding import PartitionSpec as P

EPS = 1e-06
MESH = pl.DeviceIdType.MESH
BF = jnp.bfloat16
F32 = jnp.float32
CHUNKS = 4
CAP = 5


def wait_bytes(ref, sem):
    pltpu.make_async_copy(ref, ref, sem).wait()


def relay_kernel(
    tokens, gains, ids, route_w, picks, w_gate, w_up, w_down, out,
    wgu, wd, table, tables, place, comb, hin, hnew, xs, dfirst, dout, acc, squares, hid,
    opp, side, relay, got, rout, ret, outbuf,
    wsem, tsem, hsem, dsem, agsem, rssem, retsem, osem,
    s_tab, s_tok, s_first, s_disp, s_ag, s_rs, s_ret, s_h, s_out,
):
    sec = lax.axis_index("pipe")
    rank = lax.axis_index("tensor")
    me = lax.axis_index("expert")
    last = lax.axis_size("pipe") - 1
    up1 = lax.rem(rank + 1, 4)
    dn1 = lax.rem(rank + 3, 4)
    far = lax.rem(rank + 2, 4)
    my_half = me // 4

    def send(src, dst, ssem, rsem, dev):
        pltpu.make_async_remote_copy(
            src_ref=src, dst_ref=dst, send_sem=ssem, recv_sem=rsem,
            device_id=dev, device_id_type=MESH,
        ).start()

    barrier = pltpu.get_barrier_semaphore()

    def greet(dev):
        pl.semaphore_signal(barrier, inc=1, device_id=dev, device_id_type=MESH)

    for o in range(1, 8):
        greet({"expert": lax.rem(me + o, 8)})
    greet({"tensor": up1})
    greet({"tensor": dn1})

    @pl.when(sec < last)
    def _():
        for e in range(8):
            greet({"pipe": sec + 1, "expert": e})

    @pl.when(sec > 0)
    def _():
        for e in range(8):
            greet({"pipe": sec - 1, "expert": e})

    def weight_copies():
        copies = []
        for q in range(4):
            copies.append((w_gate.at[pl.ds(q * 1024, 1024), :], wgu.at[q, :, pl.ds(0, 384)]))
            copies.append((w_up.at[pl.ds(q * 1024, 1024), :], wgu.at[q, :, pl.ds(384, 384)]))
        for q in range(4):
            copies.append((w_down.at[:, pl.ds(q * 1024, 1024)], wd.at[q]))
        return [pltpu.make_async_copy(a, b, wsem.at[i]) for i, (a, b) in enumerate(copies)]

    for copy in weight_copies():
        copy.start()

    def iota(shape, dim):
        return lax.broadcasted_iota(jnp.int32, shape, dim).astype(F32)

    def column(row, eye):
        return jnp.sum(jnp.where(eye, row, 0.0), axis=1, keepdims=True)

    sub, lane = iota((64, 64), 0), iota((64, 64), 1)
    eye = sub == lane
    shift = (lax.rem(me, 4) * 64).astype(F32)
    spread = (iota((64, 256), 0) + shift) == iota((64, 256), 1)
    row_of = iota((8, 256), 0)
    whole = jnp.zeros((8, 256), F32)
    for m in range(2):
        picked = column(picks[m : m + 1, :].astype(F32), eye)
        spot = jnp.sum(jnp.where(picked == lane, sub, 0.0), axis=0, keepdims=True)
        spot_col = column(spot, eye)
        quarter, quarter_col = jnp.floor(spot / 16.0), jnp.floor(spot_col / 16.0)
        names = [ids[m, t : t + 1, :].astype(F32) for t in range(2)]
        name_cols = [column(n, eye) for n in names]
        for t in range(2):
            slot = jnp.zeros((1, 64), F32)
            for u in range(2):
                hit = (name_cols[u] == names[t]) & (quarter_col == quarter)
                hit = hit & (spot_col * 2.0 + u < spot * 2.0 + t)
                slot = slot + jnp.sum(jnp.where(hit, 1.0, 0.0), axis=0, keepdims=True)
            at = names[t] * 80.0 + lax.rem(me, 4).astype(F32) * 20.0 + quarter * CAP + slot
            at = jnp.where(slot < CAP, at, -1.0)
            for field, value in ((t, at), (2 + t, route_w[m, t : t + 1, :])):
                placed = jnp.where(spread, column(value, eye), 0.0)
                placed = jnp.sum(placed, axis=0, keepdims=True)
                whole = whole + jnp.where(row_of == m * 4 + field, placed, 0.0)
    table[...] = whole

    greeted = 9 + jnp.where(sec < last, 8, 0) + jnp.where(sec > 0, 8, 0)
    pl.semaphore_wait(barrier, greeted)

    @pl.when(sec == 0)
    def _():
        start = pl.multiple_of(rank * 1024, 128)
        row = pl.multiple_of(lax.rem(me, 4) * 64, 64)
        for m in range(2):
            k = m * 2 + my_half
            for o in range(1, 8):
                j = lax.rem(me + o, 8)
                send(
                    tokens.at[m, :, pl.ds(pl.multiple_of(start + j * 128, 128), 128)],
                    hin.at[k, pl.ds(row, 64), :],
                    s_tok.at[m, o - 1], hsem.at[k], {"expert": j},
                )
            pltpu.make_async_copy(
                tokens.at[m, :, pl.ds(pl.multiple_of(start + me * 128, 128), 128)],
                hin.at[k, pl.ds(row, 64), :], hsem.at[k],
            ).start()

    for o in range(1, 8):
        send(table, tables.at[0, me], s_tab.at[o - 1], tsem.at[0], {"expert": lax.rem(me + o, 8)})
    pltpu.make_async_copy(table, tables.at[0, me], tsem.at[0]).start()

    @pl.when(sec > 0)
    def _():
        for e in range(8):
            send(table, tables.at[1, me], s_tab.at[7 + e], tsem.at[1], {"pipe": sec - 1, "expert": e})

    slot_rows = iota((640, 256), 0)
    slot_cols = iota((256, 640), 1)
    eye256 = iota((256, 256), 0) == iota((256, 256), 1)

    def fields(which, k, names):
        m, half = k // 2, lax.rem(k, 2)
        rows = []
        for f in names:
            at = pl.ds(m * 4 + f, 1)
            row = tables[which, half * 4, at, :]
            for i in range(1, 4):
                row = row + tables[which, half * 4 + i, at, :]
            rows.append(row)
        return rows

    def placing(which, k):
        a, b = fields(which, k, (0, 1))
        return jnp.where((slot_rows == a) | (slot_rows == b), 1.0, 0.0).astype(BF)

    def place_rows(matrix, rows, dest, k):
        moved = jnp.dot(matrix, rows, preferred_element_type=F32).astype(BF)
        for e in range(8):
            dest[k, e] = moved[e * 80 : (e + 1) * 80]

    wait_bytes(tables.at[0], tsem.at[0])

    @pl.when(sec == 0)
    def _():
        def first(k, carry):
            matrix = placing(0, k)
            wait_bytes(hin.at[k], hsem.at[k])
            place_rows(matrix, hin[k], dfirst, k)
            for o in range(1, 8):
                e = lax.rem(me + o, 8)
                send(dfirst.at[k, e], xs.at[k, 0, me], s_first.at[k], dsem.at[k, my_half], {"expert": e})
            pltpu.make_async_copy(dfirst.at[k, me], xs.at[k, 0, me], dsem.at[k, my_half]).start()
            return carry

        lax.fori_loop(0, CHUNKS, first, 0)

    def build(k, carry):
        cols = [column(row, eye256) for row in fields(0, k, (0, 1, 2, 3))]
        mix = jnp.where(slot_cols == cols[0], cols[2], 0.0)
        mix = mix + jnp.where(slot_cols == cols[1], cols[3], 0.0)
        high = mix.astype(BF)
        comb[k, 0] = high
        comb[k, 1] = (mix - high.astype(F32)).astype(BF)
        return carry

    lax.fori_loop(0, CHUNKS, build, 0)

    @pl.when(sec < last)
    def _():
        wait_bytes(tables.at[1], tsem.at[1])

        def build_next(k, carry):
            place[k] = placing(1, k)
            return carry

        lax.fori_loop(0, CHUNKS, build_next, 0)

    for copy in weight_copies():
        copy.wait()

    lo, hi = pl.ds(0, 4), pl.ds(4, 4)
    to_up, to_dn = {"tensor": up1}, {"tensor": dn1}

    def lanes(value, j):
        return value[:, j * 128 : (j + 1) * 128]

    def part(k, rel, origin):
        x = jnp.concatenate([xs[k, rel, j] for j in range(8)], axis=1).astype(F32)
        scaled = x * gains[:, pl.ds(pl.multiple_of(origin * 1024, 128), 1024)]
        both = jnp.dot(scaled.astype(BF), wgu[origin], preferred_element_type=F32)
        return jnp.sum(x * x, axis=1, keepdims=True), both

    def gather_start(k):
        ssem = s_ag.at[k]
        wait_bytes(xs.at[k, 0, lo], dsem.at[k, 0])
        send(xs.at[k, 0, lo], xs.at[k, 1, lo], ssem, agsem.at[k, 0], to_up)
        wait_bytes(xs.at[k, 0, hi], dsem.at[k, 1])
        send(xs.at[k, 0, hi], xs.at[k, 2, hi], ssem, agsem.at[k, 1], to_dn)
        send(xs.at[k, 0, lo], xs.at[k, 2, lo], ssem, agsem.at[k, 2], to_dn)
        send(xs.at[k, 0, hi], xs.at[k, 1, hi], ssem, agsem.at[k, 3], to_up)

    def gather_relay(k):
        ssem = s_ag.at[k]
        sq, both = part(k, 0, rank)
        acc[...] = both
        squares[...] = jnp.broadcast_to(sq, (80, 128))
        wait_bytes(xs.at[k, 1, lo], agsem.at[k, 0])
        send(xs.at[k, 1, lo], xs.at[k, 3, lo], ssem, agsem.at[k, 4], to_up)
        wait_bytes(xs.at[k, 2, hi], agsem.at[k, 1])
        send(xs.at[k, 2, hi], xs.at[k, 3, hi], ssem, agsem.at[k, 5], to_dn)

    def feed_forward(k):
        both, sq = acc[...], squares[:, 0:1]
        wait_bytes(xs.at[k, 1, hi], agsem.at[k, 3])
        s, b = part(k, 1, dn1)
        sq, both = sq + s, both + b
        wait_bytes(xs.at[k, 2, lo], agsem.at[k, 2])
        s, b = part(k, 2, up1)
        sq, both = sq + s, both + b
        wait_bytes(xs.at[k, 3, lo], agsem.at[k, 4])
        wait_bytes(xs.at[k, 3, hi], agsem.at[k, 5])
        s, b = part(k, 3, far)
        sq, both = sq + s, both + b
        both = both * lax.rsqrt(sq * (1.0 / 4096.0) + EPS)
        gate, up = both[:, :384], both[:, 384:]
        hid[...] = (gate / (1.0 + jnp.exp(-gate)) * up).astype(BF)

    def down(q):
        return jnp.dot(hid[...], wd[q], preferred_element_type=F32).astype(BF)

    def sum_start(k):
        ssem = s_rs.at[k]
        value = down(far)
        for j in range(8):
            opp[k, j] = lanes(value, j)
        send(opp.at[k, lo], relay.at[k, 0], ssem, rssem.at[k, 0], to_up)
        send(opp.at[k, hi], relay.at[k, 1], ssem, rssem.at[k, 1], to_dn)
        value = down(up1)
        for j in range(8):
            side[k, 0, j] = lanes(value, j)
        send(side.at[k, 0, hi], got.at[k, 0, hi], ssem, rssem.at[k, 2], to_up)
        value = down(dn1)
        for j in range(8):
            side[k, 1, j] = lanes(value, j)
        send(side.at[k, 1, lo], got.at[k, 1, lo], ssem, rssem.at[k, 3], to_dn)
        value = down(rank)
        for j in range(8):
            rout[k, j] = lanes(value, j)

    def sum_relay(k):
        ssem = s_rs.at[k]
        wait_bytes(relay.at[k, 0], rssem.at[k, 0])
        for j in range(4):
            side[k, 0, j] = (side[k, 0, j].astype(F32) + relay[k, 0, j].astype(F32)).astype(BF)
        send(side.at[k, 0, lo], got.at[k, 0, lo], ssem, rssem.at[k, 4], to_up)
        wait_bytes(relay.at[k, 1], rssem.at[k, 1])
        for j in range(4, 8):
            side[k, 1, j] = (side[k, 1, j].astype(F32) + relay[k, 1, j - 4].astype(F32)).astype(BF)
        send(side.at[k, 1, hi], got.at[k, 1, hi], ssem, rssem.at[k, 5], to_dn)

    def give_back(k, j):
        total = rout[k, j].astype(F32) + got[k, 0, j].astype(F32) + got[k, 1, j].astype(F32)
        rout[k, j] = total.astype(BF)

    def ship(k, j):
        @pl.when(me == j)
        def _():
            pltpu.make_async_copy(rout.at[k, j], ret.at[k, me], retsem.at[k]).start()

        @pl.when(me != j)
        def _():
            send(rout.at[k, j], ret.at[k, me], s_ret.at[k], retsem.at[k], {"expert": j})

    def sum_end(k):
        wait_bytes(got.at[k, 1, lo], rssem.at[k, 3])
        wait_bytes(got.at[k, 0, lo], rssem.at[k, 4])
        for j in range(4):
            give_back(k, j)
        for j in range(4):
            ship(k, j)
        wait_bytes(got.at[k, 0, hi], rssem.at[k, 2])
        wait_bytes(got.at[k, 1, hi], rssem.at[k, 5])
        for j in range(4, 8):
            give_back(k, j)
        for j in range(4, 8):
            ship(k, j)

    def home(k):
        @pl.when(sec > 0)
        def _():
            wait_bytes(hin.at[k], hsem.at[k])

        wait_bytes(ret.at[k], retsem.at[k])
        back = ret[k].reshape(640, 128)
        update = jnp.dot(comb[k, 0], back, preferred_element_type=F32)
        update = update + jnp.dot(comb[k, 1], back, preferred_element_type=F32)
        fresh = (hin[k].astype(F32) + update).astype(BF)

        @pl.when(sec < last)
        def _():
            place_rows(place[k], fresh, dout, k)
            for e in range(8):
                send(
                    dout.at[k, e], xs.at[k, 0, me], s_disp.at[k], dsem.at[k, my_half],
                    {"pipe": sec + 1, "expert": e},
                )

        hnew[k] = fresh

        @pl.when(sec < last)
        def _():
            send(hnew.at[k], hin.at[k], s_h.at[k], hsem.at[k], {"pipe": sec + 1})

        m, half = k // 2, lax.rem(k, 2)
        mine = pl.ds(pl.multiple_of(me * 128, 128), 128)
        for i in range(4):
            owner = half * 4 + i
            block = hnew.at[k, pl.ds(i * 64, 64), :]
            place_at = outbuf.at[m, :, mine]

            @pl.when(owner == me)
            def _():
                pltpu.make_async_copy(block, place_at, osem).start()

            @pl.when(owner != me)
            def _():
                send(block, place_at, s_out.at[k, i], osem, {"expert": owner})

    def turn(k, carry):
        @pl.when(k < CHUNKS)
        def _():
            gather_start(k)
            gather_relay(k)

        @pl.when(k > 0)
        def _():
            home(k - 1)

        @pl.when(k < CHUNKS)
        def _():
            feed_forward(k)
            sum_start(k)
            sum_relay(k)
            sum_end(k)

        return carry

    lax.fori_loop(0, CHUNKS + 1, turn, 0)

    for o in range(7):
        wait_bytes(table, s_tab.at[o])

    @pl.when(sec > 0)
    def _():
        for e in range(8):
            wait_bytes(table, s_tab.at[7 + e])

    @pl.when(sec == 0)
    def _():
        for m in range(2):
            for o in range(7):
                wait_bytes(hin.at[m, pl.ds(0, 64), :], s_tok.at[m, o])
        for k in range(CHUNKS):
            wait_bytes(dfirst.at[k, pl.ds(0, 7)], s_first.at[k])

    def drain(k, carry):
        wait_bytes(xs.at[k, pl.ds(0, 3)], s_ag.at[k])
        wait_bytes(xs.at[k, pl.ds(0, 3)], s_rs.at[k])
        wait_bytes(ret.at[k, pl.ds(0, 7)], s_ret.at[k])

        @pl.when(sec < last)
        def _():
            wait_bytes(dout.at[k], s_disp.at[k])
            wait_bytes(hnew.at[k], s_h.at[k])

        for i in range(4):
            owner = lax.rem(k, 2) * 4 + i

            @pl.when(owner != me)
            def _():
                wait_bytes(hnew.at[k, pl.ds(i * 64, 64), :], s_out.at[k, i])

        return carry

    lax.fori_loop(0, CHUNKS, drain, 0)
    wait_bytes(outbuf, osem)
    final = pltpu.make_async_copy(outbuf, out, wsem.at[0])
    final.start()
    final.wait()


def local(tokens, gains, route_ids, route_weights, picks, w_gate, w_up, w_down):
    vmem = pl.BlockSpec(memory_space=pltpu.VMEM)
    anywhere = pl.BlockSpec(memory_space=pl.ANY)
    dma = pltpu.SemaphoreType.DMA
    out = pl.pallas_call(
        relay_kernel,
        name="relay",
        out_shape=jax.ShapeDtypeStruct((2, 64, 1024), BF),
        in_specs=[anywhere, vmem, vmem, vmem, vmem, anywhere, anywhere, anywhere],
        out_specs=anywhere,
        scratch_shapes=[
            pltpu.VMEM((4, 1024, 768), BF),
            pltpu.VMEM((4, 384, 1024), BF),
            pltpu.VMEM((8, 256), F32),
            pltpu.VMEM((2, 8, 8, 256), F32),
            pltpu.VMEM((CHUNKS, 640, 256), BF),
            pltpu.VMEM((CHUNKS, 2, 256, 640), BF),
            pltpu.VMEM((CHUNKS, 256, 128), BF),
            pltpu.VMEM((CHUNKS, 256, 128), BF),
            pltpu.VMEM((CHUNKS, 4, 8, 80, 128), BF),
            pltpu.VMEM((CHUNKS, 8, 80, 128), BF),
            pltpu.VMEM((CHUNKS, 8, 80, 128), BF),
            pltpu.VMEM((80, 768), F32),
            pltpu.VMEM((80, 128), F32),
            pltpu.VMEM((80, 384), BF),
            pltpu.VMEM((CHUNKS, 8, 80, 128), BF),
            pltpu.VMEM((CHUNKS, 2, 8, 80, 128), BF),
            pltpu.VMEM((CHUNKS, 2, 4, 80, 128), BF),
            pltpu.VMEM((CHUNKS, 2, 8, 80, 128), BF),
            pltpu.VMEM((CHUNKS, 8, 80, 128), BF),
            pltpu.VMEM((CHUNKS, 8, 80, 128), BF),
            pltpu.VMEM((2, 64, 1024), BF),
            dma((12,)),
            dma((2,)),
            dma((CHUNKS,)),
            dma((CHUNKS, 2)),
            dma((CHUNKS, 6)),
            dma((CHUNKS, 6)),
            dma((CHUNKS,)),
            dma(()),
            dma((15,)),
            dma((2, 7)),
            dma((CHUNKS,)),
            dma((CHUNKS,)),
            dma((CHUNKS,)),
            dma((CHUNKS,)),
            dma((CHUNKS,)),
            dma((CHUNKS,)),
            dma((CHUNKS, 4)),
        ],
        compiler_params=pltpu.CompilerParams(
            collective_id=0, has_side_effects=True, vmem_limit_bytes=56 * 1024 * 1024
        ),
    )(
        tokens, gains, jnp.swapaxes(route_ids[0], 1, 2), jnp.swapaxes(route_weights[0], 1, 2),
        picks[0, :, 0], w_gate[0, 0], w_up[0, 0], w_down[0, 0],
    )
    return out[None]


def solution(mesh):
    return jax.shard_map(
        local,
        mesh=mesh,
        in_specs=(
            P(None, "expert", None),
            P("pipe", None),
            P("pipe", None, "expert", None),
            P("pipe", None, "expert", None),
            P("pipe", None, "expert", None),
            P("pipe", "expert", None, "tensor"),
            P("pipe", "expert", None, "tensor"),
            P("pipe", "expert", "tensor", None),
        ),
        out_specs=P("pipe", None, "expert", "tensor"),
        check_vma=False,
    )
```

```python
import jax
import jax.numpy as jnp
from jax import lax
from jax.experimental import pallas as pl
from jax.experimental.pallas import tpu as pltpu
from jax.sharding import PartitionSpec as P

EPS = 1e-06
MESH = pl.DeviceIdType.MESH
BF = jnp.bfloat16
F32 = jnp.float32
CHUNKS = 4
CAP = 5
PIECE = 1
PARTS = 4 // PIECE


def wait_bytes(ref, sem):
    pltpu.make_async_copy(ref, ref, sem).wait()


def relay_kernel(
    tokens, gains, ids, route_w, picks, w_gate, w_up, w_down, out,
    wgu, wd, table, tables, place, comb, hin, hnew, xs, dfirst, dout, acc, squares, hid,
    opp, side, relay, got, rout, ret, outbuf,
    wsem, tsem, hsem, dsem, agsem, rssem, retsem, osem,
    s_tab, s_tok, s_first, s_disp, s_ag, s_rs, s_ret, s_h, s_out,
):
    sec = lax.axis_index("pipe")
    rank = lax.axis_index("tensor")
    me = lax.axis_index("expert")
    last = lax.axis_size("pipe") - 1
    up1 = lax.rem(rank + 1, 4)
    dn1 = lax.rem(rank + 3, 4)
    far = lax.rem(rank + 2, 4)
    my_half = me // 4
    my_piece = me // PIECE

    def send(src, dst, ssem, rsem, dev):
        pltpu.make_async_remote_copy(
            src_ref=src, dst_ref=dst, send_sem=ssem, recv_sem=rsem,
            device_id=dev, device_id_type=MESH,
        ).start()

    barrier = pltpu.get_barrier_semaphore()

    def greet(dev):
        pl.semaphore_signal(barrier, inc=1, device_id=dev, device_id_type=MESH)

    for o in range(1, 8):
        greet({"expert": lax.rem(me + o, 8)})
    greet({"tensor": up1})
    greet({"tensor": dn1})

    @pl.when(sec < last)
    def _():
        for e in range(8):
            greet({"pipe": sec + 1, "expert": e})

    @pl.when(sec > 0)
    def _():
        for e in range(8):
            greet({"pipe": sec - 1, "expert": e})

    def weight_copies():
        copies = []
        for q in range(4):
            copies.append((w_gate.at[pl.ds(q * 1024, 1024), :], wgu.at[q, :, pl.ds(0, 384)]))
            copies.append((w_up.at[pl.ds(q * 1024, 1024), :], wgu.at[q, :, pl.ds(384, 384)]))
        for q in range(4):
            copies.append((w_down.at[:, pl.ds(q * 1024, 1024)], wd.at[q]))
        return [pltpu.make_async_copy(a, b, wsem.at[i]) for i, (a, b) in enumerate(copies)]

    for copy in weight_copies():
        copy.start()

    def iota(shape, dim):
        return lax.broadcasted_iota(jnp.int32, shape, dim).astype(F32)

    def column(row, eye):
        return jnp.sum(jnp.where(eye, row, 0.0), axis=1, keepdims=True)

    sub, lane = iota((64, 64), 0), iota((64, 64), 1)
    eye = sub == lane
    shift = (lax.rem(me, 4) * 64).astype(F32)
    spread = (iota((64, 256), 0) + shift) == iota((64, 256), 1)
    row_of = iota((8, 256), 0)
    whole = jnp.zeros((8, 256), F32)
    for m in range(2):
        picked = column(picks[m : m + 1, :].astype(F32), eye)
        spot = jnp.sum(jnp.where(picked == lane, sub, 0.0), axis=0, keepdims=True)
        spot_col = column(spot, eye)
        quarter, quarter_col = jnp.floor(spot / 16.0), jnp.floor(spot_col / 16.0)
        names = [ids[m, t : t + 1, :].astype(F32) for t in range(2)]
        name_cols = [column(n, eye) for n in names]
        for t in range(2):
            slot = jnp.zeros((1, 64), F32)
            for u in range(2):
                hit = (name_cols[u] == names[t]) & (quarter_col == quarter)
                hit = hit & (spot_col * 2.0 + u < spot * 2.0 + t)
                slot = slot + jnp.sum(jnp.where(hit, 1.0, 0.0), axis=0, keepdims=True)
            at = names[t] * 80.0 + lax.rem(me, 4).astype(F32) * 20.0 + quarter * CAP + slot
            at = jnp.where(slot < CAP, at, -1.0)
            for field, value in ((t, at), (2 + t, route_w[m, t : t + 1, :])):
                placed = jnp.where(spread, column(value, eye), 0.0)
                placed = jnp.sum(placed, axis=0, keepdims=True)
                whole = whole + jnp.where(row_of == m * 4 + field, placed, 0.0)
    table[...] = whole

    greeted = 9 + jnp.where(sec < last, 8, 0) + jnp.where(sec > 0, 8, 0)
    pl.semaphore_wait(barrier, greeted)

    @pl.when(sec == 0)
    def _():
        start = pl.multiple_of(rank * 1024, 128)
        row = pl.multiple_of(lax.rem(me, 4) * 64, 64)
        for m in range(2):
            k = m * 2 + my_half
            for o in range(1, 8):
                j = lax.rem(me + o, 8)
                send(
                    tokens.at[m, :, pl.ds(pl.multiple_of(start + j * 128, 128), 128)],
                    hin.at[k, pl.ds(row, 64), :],
                    s_tok.at[m, o - 1], hsem.at[k], {"expert": j},
                )
            pltpu.make_async_copy(
                tokens.at[m, :, pl.ds(pl.multiple_of(start + me * 128, 128), 128)],
                hin.at[k, pl.ds(row, 64), :], hsem.at[k],
            ).start()

    for o in range(1, 8):
        send(table, tables.at[0, me], s_tab.at[o - 1], tsem.at[0], {"expert": lax.rem(me + o, 8)})
    pltpu.make_async_copy(table, tables.at[0, me], tsem.at[0]).start()

    @pl.when(sec > 0)
    def _():
        for e in range(8):
            send(table, tables.at[1, me], s_tab.at[7 + e], tsem.at[1], {"pipe": sec - 1, "expert": e})

    slot_rows = iota((640, 256), 0)
    slot_cols = iota((256, 640), 1)
    eye256 = iota((256, 256), 0) == iota((256, 256), 1)

    def fields(which, k, names):
        m, half = k // 2, lax.rem(k, 2)
        rows = []
        for f in names:
            at = pl.ds(m * 4 + f, 1)
            row = tables[which, half * 4, at, :]
            for i in range(1, 4):
                row = row + tables[which, half * 4 + i, at, :]
            rows.append(row)
        return rows

    def placing(which, k):
        a, b = fields(which, k, (0, 1))
        return jnp.where((slot_rows == a) | (slot_rows == b), 1.0, 0.0).astype(BF)

    def place_rows(matrix, rows, dest, k):
        moved = jnp.dot(matrix, rows, preferred_element_type=F32).astype(BF)
        for e in range(8):
            dest[k, e] = moved[e * 80 : (e + 1) * 80]

    def first(k):
        place_rows(placing(0, k), hin[k], dfirst, k)
        for o in range(1, 8):
            e = lax.rem(me + o, 8)
            send(dfirst.at[k, e], xs.at[k, 0, me], s_first.at[k], dsem.at[k, my_piece], {"expert": e})
        pltpu.make_async_copy(dfirst.at[k, me], xs.at[k, 0, me], dsem.at[k, my_piece]).start()

    @pl.when(sec == 0)
    def _():
        wait_bytes(tables.at[0], tsem.at[0])
        wait_bytes(hin.at[0], hsem.at[0])
        first(0)

    def prepare(k):
        @pl.when((k < CHUNKS - 1) & (sec == 0))
        def _():
            wait_bytes(hin.at[k + 1], hsem.at[k + 1])
            first(k + 1)

        @pl.when((k == 0) & (sec > 0))
        def _():
            wait_bytes(tables.at[0], tsem.at[0])

        @pl.when((k == 0) & (sec < last))
        def _():
            wait_bytes(tables.at[1], tsem.at[1])

        cols = [column(row, eye256) for row in fields(0, k, (0, 1, 2, 3))]
        mix = jnp.where(slot_cols == cols[0], cols[2], 0.0)
        mix = mix + jnp.where(slot_cols == cols[1], cols[3], 0.0)
        high = mix.astype(BF)
        comb[k, 0] = high
        comb[k, 1] = (mix - high.astype(F32)).astype(BF)

        @pl.when(sec < last)
        def _():
            place[k] = placing(1, k)

        @pl.when(k == 0)
        def _():
            for copy in weight_copies():
                copy.wait()

    lo, hi = pl.ds(0, 4), pl.ds(4, 4)
    to_up, to_dn = {"tensor": up1}, {"tensor": dn1}

    def lanes(value, j):
        return value[:, j * 128 : (j + 1) * 128]

    def part(k, rel, origin):
        x = jnp.concatenate([xs[k, rel, j] for j in range(8)], axis=1).astype(F32)
        scaled = x * gains[:, pl.ds(pl.multiple_of(origin * 1024, 128), 1024)]
        both = jnp.dot(scaled.astype(BF), wgu[origin], preferred_element_type=F32)
        return jnp.sum(x * x, axis=1, keepdims=True), both

    def low(p):
        return pl.ds(p * PIECE, PIECE)

    def high_of(p):
        return pl.ds(4 + p * PIECE, PIECE)

    def gather_start(k):
        ssem = s_ag.at[k]
        for p in range(PARTS):
            wait_bytes(xs.at[k, 0, low(p)], dsem.at[k, p])
            send(xs.at[k, 0, low(p)], xs.at[k, 1, low(p)], ssem, agsem.at[k, p], to_up)
        for p in range(PARTS):
            wait_bytes(xs.at[k, 0, high_of(p)], dsem.at[k, PARTS + p])
            send(xs.at[k, 0, high_of(p)], xs.at[k, 2, high_of(p)], ssem, agsem.at[k, PARTS + p], to_dn)
        send(xs.at[k, 0, lo], xs.at[k, 2, lo], ssem, agsem.at[k, 4 * PARTS], to_dn)
        send(xs.at[k, 0, hi], xs.at[k, 1, hi], ssem, agsem.at[k, 4 * PARTS + 1], to_up)

    def gather_relay(k):
        ssem = s_ag.at[k]
        sq, both = part(k, 0, rank)
        acc[...] = both
        squares[...] = jnp.broadcast_to(sq, (80, 128))
        for p in range(PARTS):
            wait_bytes(xs.at[k, 1, low(p)], agsem.at[k, p])
            send(xs.at[k, 1, low(p)], xs.at[k, 3, low(p)], ssem, agsem.at[k, 2 * PARTS + p], to_up)
            wait_bytes(xs.at[k, 2, high_of(p)], agsem.at[k, PARTS + p])
            send(xs.at[k, 2, high_of(p)], xs.at[k, 3, high_of(p)], ssem, agsem.at[k, 3 * PARTS + p], to_dn)

    def feed_forward(k):
        both, sq = acc[...], squares[:, 0:1]
        wait_bytes(xs.at[k, 1, hi], agsem.at[k, 4 * PARTS + 1])
        s, b = part(k, 1, dn1)
        sq, both = sq + s, both + b
        wait_bytes(xs.at[k, 2, lo], agsem.at[k, 4 * PARTS])
        s, b = part(k, 2, up1)
        sq, both = sq + s, both + b
        for p in range(PARTS):
            wait_bytes(xs.at[k, 3, low(p)], agsem.at[k, 2 * PARTS + p])
            wait_bytes(xs.at[k, 3, high_of(p)], agsem.at[k, 3 * PARTS + p])
        s, b = part(k, 3, far)
        sq, both = sq + s, both + b
        both = both * lax.rsqrt(sq * (1.0 / 4096.0) + EPS)
        gate, up = both[:, :384], both[:, 384:]
        hid[...] = (gate / (1.0 + jnp.exp(-gate)) * up).astype(BF)

    def down(q):
        return jnp.dot(hid[...], wd[q], preferred_element_type=F32).astype(BF)

    def sum_start(k):
        ssem = s_rs.at[k]
        value = down(far)
        for j in range(8):
            opp[k, j] = lanes(value, j)
        for p in range(PARTS):
            send(opp.at[k, low(p)], relay.at[k, 0, low(p)], ssem, rssem.at[k, p], to_up)
            send(opp.at[k, high_of(p)], relay.at[k, 1, low(p)], ssem, rssem.at[k, PARTS + p], to_dn)
        value = down(up1)
        for j in range(8):
            side[k, 0, j] = lanes(value, j)
        send(side.at[k, 0, hi], got.at[k, 0, hi], ssem, rssem.at[k, 4 * PARTS], to_up)
        value = down(dn1)
        for j in range(8):
            side[k, 1, j] = lanes(value, j)
        send(side.at[k, 1, lo], got.at[k, 1, lo], ssem, rssem.at[k, 4 * PARTS + 1], to_dn)
        value = down(rank)
        for j in range(8):
            rout[k, j] = lanes(value, j)

    def sum_relay(k):
        ssem = s_rs.at[k]
        for p in range(PARTS):
            wait_bytes(relay.at[k, 0, low(p)], rssem.at[k, p])
            for j in range(p * PIECE, (p + 1) * PIECE):
                side[k, 0, j] = (side[k, 0, j].astype(F32) + relay[k, 0, j].astype(F32)).astype(BF)
            send(side.at[k, 0, low(p)], got.at[k, 0, low(p)], ssem, rssem.at[k, 2 * PARTS + p], to_up)
            wait_bytes(relay.at[k, 1, low(p)], rssem.at[k, PARTS + p])
            for j in range(p * PIECE, (p + 1) * PIECE):
                side[k, 1, 4 + j] = (side[k, 1, 4 + j].astype(F32) + relay[k, 1, j].astype(F32)).astype(BF)
            send(side.at[k, 1, high_of(p)], got.at[k, 1, high_of(p)], ssem, rssem.at[k, 3 * PARTS + p], to_dn)

    def give_back(k, j):
        total = rout[k, j].astype(F32) + got[k, 0, j].astype(F32) + got[k, 1, j].astype(F32)
        rout[k, j] = total.astype(BF)

    def ship(k, j):
        @pl.when(me == j)
        def _():
            pltpu.make_async_copy(rout.at[k, j], ret.at[k, me], retsem.at[k]).start()

        @pl.when(me != j)
        def _():
            send(rout.at[k, j], ret.at[k, me], s_ret.at[k], retsem.at[k], {"expert": j})

    def sum_end(k):
        wait_bytes(got.at[k, 1, lo], rssem.at[k, 4 * PARTS + 1])
        wait_bytes(got.at[k, 0, hi], rssem.at[k, 4 * PARTS])
        for p in range(PARTS):
            for begin, which in ((p * PIECE, 0), (4 + p * PIECE, 1)):
                wait_bytes(got.at[k, which, pl.ds(begin, PIECE)], rssem.at[k, (2 + which) * PARTS + p])
                for j in range(begin, begin + PIECE):
                    give_back(k, j)
                for j in range(begin, begin + PIECE):
                    ship(k, j)

    def home(k):
        @pl.when(sec > 0)
        def _():
            wait_bytes(hin.at[k], hsem.at[k])

        wait_bytes(ret.at[k], retsem.at[k])
        back = ret[k].reshape(640, 128)
        update = jnp.dot(comb[k, 0], back, preferred_element_type=F32)
        update = update + jnp.dot(comb[k, 1], back, preferred_element_type=F32)
        fresh = (hin[k].astype(F32) + update).astype(BF)

        @pl.when(sec < last)
        def _():
            place_rows(place[k], fresh, dout, k)
            for e in range(8):
                send(
                    dout.at[k, e], xs.at[k, 0, me], s_disp.at[k], dsem.at[k, my_piece],
                    {"pipe": sec + 1, "expert": e},
                )

        hnew[k] = fresh

        @pl.when(sec < last)
        def _():
            send(hnew.at[k], hin.at[k], s_h.at[k], hsem.at[k], {"pipe": sec + 1})

        m, half = k // 2, lax.rem(k, 2)
        mine = pl.ds(pl.multiple_of(me * 128, 128), 128)
        for i in range(4):
            owner = half * 4 + i
            block = hnew.at[k, pl.ds(i * 64, 64), :]
            place_at = outbuf.at[m, :, mine]

            @pl.when(owner == me)
            def _():
                pltpu.make_async_copy(block, place_at, osem).start()

            @pl.when(owner != me)
            def _():
                send(block, place_at, s_out.at[k, i], osem, {"expert": owner})

    def turn(k, carry):
        @pl.when((k < CHUNKS))
        def _():
            gather_start(k)
            prepare(k)

        @pl.when((k >= 1))
        def _():
            sum_end(k - 1)

        @pl.when((k < CHUNKS))
        def _():
            gather_relay(k)

        @pl.when((k >= 1))
        def _():
            home(k - 1)

        @pl.when((k < CHUNKS))
        def _():
            feed_forward(k)
            sum_start(k)
            sum_relay(k)

        return carry

    lax.fori_loop(0, CHUNKS + 1, turn, 0)

    for o in range(7):
        wait_bytes(table, s_tab.at[o])

    @pl.when(sec > 0)
    def _():
        for e in range(8):
            wait_bytes(table, s_tab.at[7 + e])

    @pl.when(sec == 0)
    def _():
        for m in range(2):
            for o in range(7):
                wait_bytes(hin.at[m, pl.ds(0, 64), :], s_tok.at[m, o])
        for k in range(CHUNKS):
            wait_bytes(dfirst.at[k, pl.ds(0, 7)], s_first.at[k])

    def drain(k, carry):
        wait_bytes(xs.at[k, pl.ds(0, 3)], s_ag.at[k])
        wait_bytes(xs.at[k, pl.ds(0, 3)], s_rs.at[k])
        wait_bytes(ret.at[k, pl.ds(0, 7)], s_ret.at[k])

        @pl.when(sec < last)
        def _():
            wait_bytes(dout.at[k], s_disp.at[k])
            wait_bytes(hnew.at[k], s_h.at[k])

        for i in range(4):
            owner = lax.rem(k, 2) * 4 + i

            @pl.when(owner != me)
            def _():
                wait_bytes(hnew.at[k, pl.ds(i * 64, 64), :], s_out.at[k, i])

        return carry

    lax.fori_loop(0, CHUNKS, drain, 0)
    wait_bytes(outbuf, osem)
    final = pltpu.make_async_copy(outbuf, out, wsem.at[0])
    final.start()
    final.wait()


def local(tokens, gains, route_ids, route_weights, picks, w_gate, w_up, w_down):
    vmem = pl.BlockSpec(memory_space=pltpu.VMEM)
    anywhere = pl.BlockSpec(memory_space=pl.ANY)
    dma = pltpu.SemaphoreType.DMA
    out = pl.pallas_call(
        relay_kernel,
        name="relay",
        out_shape=jax.ShapeDtypeStruct((2, 64, 1024), BF),
        in_specs=[anywhere, vmem, vmem, vmem, vmem, anywhere, anywhere, anywhere],
        out_specs=anywhere,
        scratch_shapes=[
            pltpu.VMEM((4, 1024, 768), BF),
            pltpu.VMEM((4, 384, 1024), BF),
            pltpu.VMEM((8, 256), F32),
            pltpu.VMEM((2, 8, 8, 256), F32),
            pltpu.VMEM((CHUNKS, 640, 256), BF),
            pltpu.VMEM((CHUNKS, 2, 256, 640), BF),
            pltpu.VMEM((CHUNKS, 256, 128), BF),
            pltpu.VMEM((CHUNKS, 256, 128), BF),
            pltpu.VMEM((CHUNKS, 4, 8, 80, 128), BF),
            pltpu.VMEM((CHUNKS, 8, 80, 128), BF),
            pltpu.VMEM((CHUNKS, 8, 80, 128), BF),
            pltpu.VMEM((80, 768), F32),
            pltpu.VMEM((80, 128), F32),
            pltpu.VMEM((80, 384), BF),
            pltpu.VMEM((CHUNKS, 8, 80, 128), BF),
            pltpu.VMEM((CHUNKS, 2, 8, 80, 128), BF),
            pltpu.VMEM((CHUNKS, 2, 4, 80, 128), BF),
            pltpu.VMEM((CHUNKS, 2, 8, 80, 128), BF),
            pltpu.VMEM((CHUNKS, 8, 80, 128), BF),
            pltpu.VMEM((CHUNKS, 8, 80, 128), BF),
            pltpu.VMEM((2, 64, 1024), BF),
            dma((12,)),
            dma((2,)),
            dma((CHUNKS,)),
            dma((CHUNKS, 2 * PARTS)),
            dma((CHUNKS, 4 * PARTS + 2)),
            dma((CHUNKS, 4 * PARTS + 2)),
            dma((CHUNKS,)),
            dma(()),
            dma((15,)),
            dma((2, 7)),
            dma((CHUNKS,)),
            dma((CHUNKS,)),
            dma((CHUNKS,)),
            dma((CHUNKS,)),
            dma((CHUNKS,)),
            dma((CHUNKS,)),
            dma((CHUNKS, 4)),
        ],
        compiler_params=pltpu.CompilerParams(
            collective_id=0, has_side_effects=True, vmem_limit_bytes=56 * 1024 * 1024
        ),
    )(
        tokens, gains, jnp.swapaxes(route_ids[0], 1, 2), jnp.swapaxes(route_weights[0], 1, 2),
        picks[0, :, 0], w_gate[0, 0], w_up[0, 0], w_down[0, 0],
    )
    return out[None]


def solution(mesh):
    return jax.shard_map(
        local,
        mesh=mesh,
        in_specs=(
            P(None, "expert", None),
            P("pipe", None),
            P("pipe", None, "expert", None),
            P("pipe", None, "expert", None),
            P("pipe", None, "expert", None),
            P("pipe", "expert", None, "tensor"),
            P("pipe", "expert", None, "tensor"),
            P("pipe", "expert", "tensor", None),
        ),
        out_specs=P("pipe", None, "expert", "tensor"),
        check_vma=False,
    )
```

```python
import jax
import jax.numpy as jnp
from jax import lax
from jax.experimental import pallas as pl
from jax.experimental.pallas import tpu as pltpu
from jax.sharding import PartitionSpec as P

EPS = 1e-06
MESH = pl.DeviceIdType.MESH
BF = jnp.bfloat16
F32 = jnp.float32
CHUNKS = 4
CAP = 5
PIECE = 1
PARTS = 4 // PIECE


def wait_bytes(ref, sem):
    pltpu.make_async_copy(ref, ref, sem).wait()


def relay_kernel(
    tokens, gains, ids, route_w, picks, w_gate, w_up, w_down, out,
    wgu, wd, table, tables, place, comb, hin, hnew, xs, dfirst, dout, acc, squares, hid, total, relay_w,
    opp, side, relay, got, rout, ret, outbuf,
    wsem, dwsem, tsem, hsem, dsem, agsem, rssem, retsem, osem,
    s_tab, s_dw, s_tok, s_first, s_disp, s_ag, s_rs, s_ret, s_h, s_out,
):
    sec = lax.axis_index("pipe")
    rank = lax.axis_index("tensor")
    me = lax.axis_index("expert")
    last = lax.axis_size("pipe") - 1
    up1 = lax.rem(rank + 1, 4)
    dn1 = lax.rem(rank + 3, 4)
    far = lax.rem(rank + 2, 4)
    my_half = me // 4
    my_piece = me // PIECE

    def send(src, dst, ssem, rsem, dev):
        pltpu.make_async_remote_copy(
            src_ref=src, dst_ref=dst, send_sem=ssem, recv_sem=rsem,
            device_id=dev, device_id_type=MESH,
        ).start()

    barrier = pltpu.get_barrier_semaphore()

    def greet(dev):
        pl.semaphore_signal(barrier, inc=1, device_id=dev, device_id_type=MESH)

    for o in range(1, 8):
        greet({"expert": lax.rem(me + o, 8)})
    greet({"tensor": up1})
    greet({"tensor": dn1})
    greet({"tensor": far})

    @pl.when(sec < last)
    def _():
        for e in range(8):
            greet({"pipe": sec + 1, "expert": e})

    @pl.when(sec > 0)
    def _():
        for e in range(8):
            greet({"pipe": sec - 1, "expert": e})

    def weight_copies():
        copies = []
        for q in range(4):
            copies.append((w_gate.at[pl.ds(q * 1024, 1024), :], wgu.at[q, :, pl.ds(0, 384)]))
            copies.append((w_up.at[pl.ds(q * 1024, 1024), :], wgu.at[q, :, pl.ds(384, 384)]))
        return [pltpu.make_async_copy(a, b, wsem.at[i]) for i, (a, b) in enumerate(copies)]

    def slice_of_down(q):
        return w_down.at[:, pl.ds(pl.multiple_of(q * 1024, 128), 1024)]

    def first_down_copies():
        return [pltpu.make_async_copy(slice_of_down(q), wd.at[q], wsem.at[8 + q]) for q in range(4)]

    def own_down_copy():
        return pltpu.make_async_copy(slice_of_down(rank), wd.at[rank], wsem.at[8])

    for copy in weight_copies():
        copy.start()

    @pl.when(sec == 0)
    def _():
        for copy in first_down_copies():
            copy.start()

    @pl.when(sec > 0)
    def _():
        own_down_copy().start()

    def iota(shape, dim):
        return lax.broadcasted_iota(jnp.int32, shape, dim).astype(F32)

    def column(row, eye):
        return jnp.sum(jnp.where(eye, row, 0.0), axis=1, keepdims=True)

    sub, lane = iota((64, 64), 0), iota((64, 64), 1)
    eye = sub == lane
    shift = (lax.rem(me, 4) * 64).astype(F32)
    spread = (iota((64, 256), 0) + shift) == iota((64, 256), 1)
    row_of = iota((8, 256), 0)
    whole = jnp.zeros((8, 256), F32)
    for m in range(2):
        picked = column(picks[m : m + 1, :].astype(F32), eye)
        spot = jnp.sum(jnp.where(picked == lane, sub, 0.0), axis=0, keepdims=True)
        spot_col = column(spot, eye)
        quarter, quarter_col = jnp.floor(spot / 16.0), jnp.floor(spot_col / 16.0)
        names = [ids[m, t : t + 1, :].astype(F32) for t in range(2)]
        name_cols = [column(n, eye) for n in names]
        for t in range(2):
            slot = jnp.zeros((1, 64), F32)
            for u in range(2):
                hit = (name_cols[u] == names[t]) & (quarter_col == quarter)
                hit = hit & (spot_col * 2.0 + u < spot * 2.0 + t)
                slot = slot + jnp.sum(jnp.where(hit, 1.0, 0.0), axis=0, keepdims=True)
            at = names[t] * 80.0 + lax.rem(me, 4).astype(F32) * 20.0 + quarter * CAP + slot
            at = jnp.where(slot < CAP, at, -1.0)
            for field, value in ((t, at), (2 + t, route_w[m, t : t + 1, :])):
                placed = jnp.where(spread, column(value, eye), 0.0)
                placed = jnp.sum(placed, axis=0, keepdims=True)
                whole = whole + jnp.where(row_of == m * 4 + field, placed, 0.0)
    table[...] = whole

    greeted = 10 + jnp.where(sec < last, 8, 0) + jnp.where(sec > 0, 8, 0)
    pl.semaphore_wait(barrier, greeted)

    @pl.when(sec == 0)
    def _():
        start = pl.multiple_of(rank * 1024, 128)
        row = pl.multiple_of(lax.rem(me, 4) * 64, 64)
        for m in range(2):
            k = m * 2 + my_half
            for o in range(1, 8):
                j = lax.rem(me + o, 8)
                send(
                    tokens.at[m, :, pl.ds(pl.multiple_of(start + j * 128, 128), 128)],
                    hin.at[k, pl.ds(row, 64), :],
                    s_tok.at[m, o - 1], hsem.at[k], {"expert": j},
                )
            pltpu.make_async_copy(
                tokens.at[m, :, pl.ds(pl.multiple_of(start + me * 128, 128), 128)],
                hin.at[k, pl.ds(row, 64), :], hsem.at[k],
            ).start()

    for o in range(1, 8):
        send(table, tables.at[0, me], s_tab.at[o - 1], tsem.at[0], {"expert": lax.rem(me + o, 8)})
    pltpu.make_async_copy(table, tables.at[0, me], tsem.at[0]).start()

    @pl.when(sec > 0)
    def _():
        for e in range(8):
            send(table, tables.at[1, me], s_tab.at[7 + e], tsem.at[1], {"pipe": sec - 1, "expert": e})

    to_up, to_dn = {"tensor": up1}, {"tensor": dn1}
    top, rest = pl.ds(0, 192), pl.ds(192, 192)

    @pl.when(sec > 0)
    def _():
        distant = pl.ds(pl.multiple_of(far * 1024, 128), 1024)
        send(w_down.at[top, distant], relay_w.at[0], s_dw.at[0], dwsem.at[2], to_up)
        send(w_down.at[rest, distant], relay_w.at[1], s_dw.at[1], dwsem.at[3], to_dn)
        send(slice_of_down(up1), wd.at[rank], s_dw.at[2], dwsem.at[0], to_up)
        send(slice_of_down(dn1), wd.at[rank], s_dw.at[3], dwsem.at[1], to_dn)
        wait_bytes(relay_w.at[0], dwsem.at[2])
        send(relay_w.at[0], wd.at[dn1, top], s_dw.at[4], dwsem.at[4], to_up)
        wait_bytes(relay_w.at[1], dwsem.at[3])
        send(relay_w.at[1], wd.at[up1, rest], s_dw.at[5], dwsem.at[5], to_dn)

    slot_rows = iota((640, 256), 0)
    slot_cols = iota((256, 640), 1)
    eye256 = iota((256, 256), 0) == iota((256, 256), 1)

    def fields(which, k, names):
        m, half = k // 2, lax.rem(k, 2)
        rows = []
        for f in names:
            at = pl.ds(m * 4 + f, 1)
            row = tables[which, half * 4, at, :]
            for i in range(1, 4):
                row = row + tables[which, half * 4 + i, at, :]
            rows.append(row)
        return rows

    def placing(which, k):
        a, b = fields(which, k, (0, 1))
        return jnp.where((slot_rows == a) | (slot_rows == b), 1.0, 0.0).astype(BF)

    def place_rows(matrix, rows, dest, k):
        moved = jnp.dot(matrix, rows, preferred_element_type=F32).astype(BF)
        for e in range(8):
            dest[k, e] = moved[e * 80 : (e + 1) * 80]

    def first(k):
        place_rows(placing(0, k), hin[k], dfirst, k)
        for o in range(1, 8):
            e = lax.rem(me + o, 8)
            send(dfirst.at[k, e], xs.at[k, 0, me], s_first.at[k], dsem.at[k, my_piece], {"expert": e})
        pltpu.make_async_copy(dfirst.at[k, me], xs.at[k, 0, me], dsem.at[k, my_piece]).start()

    @pl.when(sec == 0)
    def _():
        wait_bytes(tables.at[0], tsem.at[0])
        wait_bytes(hin.at[0], hsem.at[0])
        first(0)

    def prepare(k):
        @pl.when((k < CHUNKS - 1) & (sec == 0))
        def _():
            wait_bytes(hin.at[k + 1], hsem.at[k + 1])
            first(k + 1)

        @pl.when((k == 0) & (sec > 0))
        def _():
            wait_bytes(tables.at[0], tsem.at[0])

        @pl.when((k == 0) & (sec < last))
        def _():
            wait_bytes(tables.at[1], tsem.at[1])

        cols = [column(row, eye256) for row in fields(0, k, (0, 1, 2, 3))]
        mix = jnp.where(slot_cols == cols[0], cols[2], 0.0)
        mix = mix + jnp.where(slot_cols == cols[1], cols[3], 0.0)
        high = mix.astype(BF)
        comb[k, 0] = high
        comb[k, 1] = (mix - high.astype(F32)).astype(BF)

        @pl.when(sec < last)
        def _():
            place[k] = placing(1, k)

        @pl.when(k == 0)
        def _():
            for copy in weight_copies():
                copy.wait()

        @pl.when((k == 0) & (sec == 0))
        def _():
            for copy in first_down_copies():
                copy.wait()

        @pl.when((k == 0) & (sec > 0))
        def _():
            own_down_copy().wait()
            wait_bytes(wd.at[dn1], dwsem.at[0])
            wait_bytes(wd.at[up1], dwsem.at[1])
            wait_bytes(wd.at[far, top], dwsem.at[4])
            wait_bytes(wd.at[far, rest], dwsem.at[5])

    lo, hi = pl.ds(0, 4), pl.ds(4, 4)

    def lanes(value, j):
        return value[:, j * 128 : (j + 1) * 128]

    def part(k, rel, origin):
        x = jnp.concatenate([xs[k, rel, j] for j in range(8)], axis=1).astype(F32)
        scaled = x * gains[:, pl.ds(pl.multiple_of(origin * 1024, 128), 1024)]
        both = jnp.dot(scaled.astype(BF), wgu[origin], preferred_element_type=F32)
        return jnp.sum(x * x, axis=1, keepdims=True), both

    def low(p):
        return pl.ds(p * PIECE, PIECE)

    def high_of(p):
        return pl.ds(4 + p * PIECE, PIECE)

    def gather_start(k):
        ssem = s_ag.at[k]
        for p in range(PARTS):
            wait_bytes(xs.at[k, 0, low(p)], dsem.at[k, p])
            send(xs.at[k, 0, low(p)], xs.at[k, 1, low(p)], ssem, agsem.at[k, p], to_up)
        for p in range(PARTS):
            wait_bytes(xs.at[k, 0, high_of(p)], dsem.at[k, PARTS + p])
            send(xs.at[k, 0, high_of(p)], xs.at[k, 2, high_of(p)], ssem, agsem.at[k, PARTS + p], to_dn)
        send(xs.at[k, 0, lo], xs.at[k, 2, lo], ssem, agsem.at[k, 4 * PARTS], to_dn)
        send(xs.at[k, 0, hi], xs.at[k, 1, hi], ssem, agsem.at[k, 4 * PARTS + 1], to_up)

    def gather_relay(k):
        ssem = s_ag.at[k]
        sq, both = part(k, 0, rank)
        acc[...] = both
        squares[...] = jnp.broadcast_to(sq, (80, 128))
        for p in range(PARTS):
            wait_bytes(xs.at[k, 1, low(p)], agsem.at[k, p])
            send(xs.at[k, 1, low(p)], xs.at[k, 3, low(p)], ssem, agsem.at[k, 2 * PARTS + p], to_up)
            wait_bytes(xs.at[k, 2, high_of(p)], agsem.at[k, PARTS + p])
            send(xs.at[k, 2, high_of(p)], xs.at[k, 3, high_of(p)], ssem, agsem.at[k, 3 * PARTS + p], to_dn)

    def feed_forward(k):
        both, sq = acc[...], squares[:, 0:1]
        wait_bytes(xs.at[k, 1, hi], agsem.at[k, 4 * PARTS + 1])
        s, b = part(k, 1, dn1)
        sq, both = sq + s, both + b
        wait_bytes(xs.at[k, 2, lo], agsem.at[k, 4 * PARTS])
        s, b = part(k, 2, up1)
        sq, both = sq + s, both + b
        for p in range(PARTS):
            wait_bytes(xs.at[k, 3, low(p)], agsem.at[k, 2 * PARTS + p])
            wait_bytes(xs.at[k, 3, high_of(p)], agsem.at[k, 3 * PARTS + p])
        s, b = part(k, 3, far)
        sq, both = sq + s, both + b
        both = both * lax.rsqrt(sq * (1.0 / 4096.0) + EPS)
        gate, up = both[:, :384], both[:, 384:]
        hid[k, 0] = (gate / (1.0 + jnp.exp(-gate)) * up).astype(BF)

    def down(k, q):
        return jnp.dot(hid[k, 0], wd[q], preferred_element_type=F32).astype(BF)

    def spread_start(k):
        ssem = s_rs.at[k]
        send(hid.at[k, 0], hid.at[k, 3], ssem, rssem.at[k, 2], {"tensor": far})
        send(hid.at[k, 0], hid.at[k, 1], ssem, rssem.at[k, 0], to_up)
        send(hid.at[k, 0], hid.at[k, 2], ssem, rssem.at[k, 1], to_dn)
        total[...] = jnp.dot(hid[k, 0], wd[rank], preferred_element_type=F32)

    def spread_end(k):
        wait_bytes(hid.at[k, 1], rssem.at[k, 0])
        total[...] += jnp.dot(hid[k, 1], wd[dn1], preferred_element_type=F32)
        wait_bytes(hid.at[k, 2], rssem.at[k, 1])
        total[...] += jnp.dot(hid[k, 2], wd[up1], preferred_element_type=F32)
        wait_bytes(hid.at[k, 3], rssem.at[k, 2])
        done = (total[...] + jnp.dot(hid[k, 3], wd[far], preferred_element_type=F32)).astype(BF)
        for j in range(8):
            rout[k, j] = lanes(done, j)
        for j in range(8):
            ship(k, j)

    def first_layer_sum_start(k):
        ssem = s_rs.at[k]
        value = down(k, far)
        for j in range(8):
            opp[k, j] = lanes(value, j)
        for p in range(PARTS):
            send(opp.at[k, low(p)], relay.at[k, 0, low(p)], ssem, rssem.at[k, p], to_up)
            send(opp.at[k, high_of(p)], relay.at[k, 1, low(p)], ssem, rssem.at[k, PARTS + p], to_dn)
        value = down(k, up1)
        for j in range(8):
            side[k, 0, j] = lanes(value, j)
        send(side.at[k, 0, hi], got.at[k, 0, hi], ssem, rssem.at[k, 4 * PARTS], to_up)
        value = down(k, dn1)
        for j in range(8):
            side[k, 1, j] = lanes(value, j)
        send(side.at[k, 1, lo], got.at[k, 1, lo], ssem, rssem.at[k, 4 * PARTS + 1], to_dn)
        value = down(k, rank)
        for j in range(8):
            rout[k, j] = lanes(value, j)

    def first_layer_sum_relay(k):
        ssem = s_rs.at[k]
        for p in range(PARTS):
            wait_bytes(relay.at[k, 0, low(p)], rssem.at[k, p])
            for j in range(p * PIECE, (p + 1) * PIECE):
                side[k, 0, j] = (side[k, 0, j].astype(F32) + relay[k, 0, j].astype(F32)).astype(BF)
            send(side.at[k, 0, low(p)], got.at[k, 0, low(p)], ssem, rssem.at[k, 2 * PARTS + p], to_up)
            wait_bytes(relay.at[k, 1, low(p)], rssem.at[k, PARTS + p])
            for j in range(p * PIECE, (p + 1) * PIECE):
                side[k, 1, 4 + j] = (side[k, 1, 4 + j].astype(F32) + relay[k, 1, j].astype(F32)).astype(BF)
            send(side.at[k, 1, high_of(p)], got.at[k, 1, high_of(p)], ssem, rssem.at[k, 3 * PARTS + p], to_dn)

    def give_back(k, j):
        total = rout[k, j].astype(F32) + got[k, 0, j].astype(F32) + got[k, 1, j].astype(F32)
        rout[k, j] = total.astype(BF)

    def ship(k, j):
        @pl.when(me == j)
        def _():
            pltpu.make_async_copy(rout.at[k, j], ret.at[k, me], retsem.at[k]).start()

        @pl.when(me != j)
        def _():
            send(rout.at[k, j], ret.at[k, me], s_ret.at[k], retsem.at[k], {"expert": j})

    def first_layer_sum_end(k):
        wait_bytes(got.at[k, 1, lo], rssem.at[k, 4 * PARTS + 1])
        wait_bytes(got.at[k, 0, hi], rssem.at[k, 4 * PARTS])
        for p in range(PARTS):
            for begin, which in ((p * PIECE, 0), (4 + p * PIECE, 1)):
                wait_bytes(got.at[k, which, pl.ds(begin, PIECE)], rssem.at[k, (2 + which) * PARTS + p])
                for j in range(begin, begin + PIECE):
                    give_back(k, j)
                for j in range(begin, begin + PIECE):
                    ship(k, j)

    def sum_start(k):
        @pl.when(sec == 0)
        def _():
            first_layer_sum_start(k)

        @pl.when(sec > 0)
        def _():
            spread_start(k)

    def sum_relay(k):
        @pl.when(sec == 0)
        def _():
            first_layer_sum_relay(k)

    def sum_end(k):
        @pl.when(sec == 0)
        def _():
            first_layer_sum_end(k)

        @pl.when(sec > 0)
        def _():
            spread_end(k)

    def home(k):
        @pl.when(sec > 0)
        def _():
            wait_bytes(hin.at[k], hsem.at[k])

        wait_bytes(ret.at[k], retsem.at[k])
        back = ret[k].reshape(640, 128)
        update = jnp.dot(comb[k, 0], back, preferred_element_type=F32)
        update = update + jnp.dot(comb[k, 1], back, preferred_element_type=F32)
        fresh = (hin[k].astype(F32) + update).astype(BF)

        @pl.when(sec < last)
        def _():
            place_rows(place[k], fresh, dout, k)
            for e in range(8):
                send(
                    dout.at[k, e], xs.at[k, 0, me], s_disp.at[k], dsem.at[k, my_piece],
                    {"pipe": sec + 1, "expert": e},
                )

        hnew[k] = fresh

        @pl.when(sec < last)
        def _():
            send(hnew.at[k], hin.at[k], s_h.at[k], hsem.at[k], {"pipe": sec + 1})

        m, half = k // 2, lax.rem(k, 2)
        mine = pl.ds(pl.multiple_of(me * 128, 128), 128)
        for i in range(4):
            owner = half * 4 + i
            block = hnew.at[k, pl.ds(i * 64, 64), :]
            place_at = outbuf.at[m, :, mine]

            @pl.when(owner == me)
            def _():
                pltpu.make_async_copy(block, place_at, osem).start()

            @pl.when(owner != me)
            def _():
                send(block, place_at, s_out.at[k, i], osem, {"expert": owner})

    def turn(k, carry):
        @pl.when((k < CHUNKS))
        def _():
            gather_start(k)
            prepare(k)
            gather_relay(k)

        @pl.when((k >= 1))
        def _():
            home(k - 1)

        @pl.when((k < CHUNKS))
        def _():
            feed_forward(k)
            sum_start(k)
            sum_relay(k)
            sum_end(k)

        return carry

    lax.fori_loop(0, CHUNKS + 1, turn, 0)

    for o in range(7):
        wait_bytes(table, s_tab.at[o])

    @pl.when(sec > 0)
    def _():
        for e in range(8):
            wait_bytes(table, s_tab.at[7 + e])
        for i in range(4):
            wait_bytes(relay_w.at[0] if i < 2 else wd.at[0], s_dw.at[i])
        for i in range(2):
            wait_bytes(relay_w.at[i], s_dw.at[4 + i])

    @pl.when(sec == 0)
    def _():
        for m in range(2):
            for o in range(7):
                wait_bytes(hin.at[m, pl.ds(0, 64), :], s_tok.at[m, o])
        for k in range(CHUNKS):
            wait_bytes(dfirst.at[k, pl.ds(0, 7)], s_first.at[k])

    def drain(k, carry):
        wait_bytes(xs.at[k, pl.ds(0, 3)], s_ag.at[k])

        @pl.when(sec == 0)
        def _():
            wait_bytes(xs.at[k, pl.ds(0, 3)], s_rs.at[k])

        @pl.when(sec > 0)
        def _():
            wait_bytes(hid.at[k, pl.ds(0, 3)], s_rs.at[k])

        wait_bytes(ret.at[k, pl.ds(0, 7)], s_ret.at[k])

        @pl.when(sec < last)
        def _():
            wait_bytes(dout.at[k], s_disp.at[k])
            wait_bytes(hnew.at[k], s_h.at[k])

        for i in range(4):
            owner = lax.rem(k, 2) * 4 + i

            @pl.when(owner != me)
            def _():
                wait_bytes(hnew.at[k, pl.ds(i * 64, 64), :], s_out.at[k, i])

        return carry

    lax.fori_loop(0, CHUNKS, drain, 0)
    wait_bytes(outbuf, osem)
    final = pltpu.make_async_copy(outbuf, out, wsem.at[0])
    final.start()
    final.wait()


def local(tokens, gains, route_ids, route_weights, picks, w_gate, w_up, w_down):
    vmem = pl.BlockSpec(memory_space=pltpu.VMEM)
    anywhere = pl.BlockSpec(memory_space=pl.ANY)
    dma = pltpu.SemaphoreType.DMA
    out = pl.pallas_call(
        relay_kernel,
        name="relay",
        out_shape=jax.ShapeDtypeStruct((2, 64, 1024), BF),
        in_specs=[anywhere, vmem, vmem, vmem, vmem, anywhere, anywhere, anywhere],
        out_specs=anywhere,
        scratch_shapes=[
            pltpu.VMEM((4, 1024, 768), BF),
            pltpu.VMEM((4, 384, 1024), BF),
            pltpu.VMEM((8, 256), F32),
            pltpu.VMEM((2, 8, 8, 256), F32),
            pltpu.VMEM((CHUNKS, 640, 256), BF),
            pltpu.VMEM((CHUNKS, 2, 256, 640), BF),
            pltpu.VMEM((CHUNKS, 256, 128), BF),
            pltpu.VMEM((CHUNKS, 256, 128), BF),
            pltpu.VMEM((CHUNKS, 4, 8, 80, 128), BF),
            pltpu.VMEM((CHUNKS, 8, 80, 128), BF),
            pltpu.VMEM((CHUNKS, 8, 80, 128), BF),
            pltpu.VMEM((80, 768), F32),
            pltpu.VMEM((80, 128), F32),
            pltpu.VMEM((CHUNKS, 4, 80, 384), BF),
            pltpu.VMEM((80, 1024), F32),
            pltpu.VMEM((2, 192, 1024), BF),
            pltpu.VMEM((CHUNKS, 8, 80, 128), BF),
            pltpu.VMEM((CHUNKS, 2, 8, 80, 128), BF),
            pltpu.VMEM((CHUNKS, 2, 4, 80, 128), BF),
            pltpu.VMEM((CHUNKS, 2, 8, 80, 128), BF),
            pltpu.VMEM((CHUNKS, 8, 80, 128), BF),
            pltpu.VMEM((CHUNKS, 8, 80, 128), BF),
            pltpu.VMEM((2, 64, 1024), BF),
            dma((12,)),
            dma((6,)),
            dma((2,)),
            dma((CHUNKS,)),
            dma((CHUNKS, 2 * PARTS)),
            dma((CHUNKS, 4 * PARTS + 2)),
            dma((CHUNKS, 4 * PARTS + 2)),
            dma((CHUNKS,)),
            dma(()),
            dma((15,)),
            dma((6,)),
            dma((2, 7)),
            dma((CHUNKS,)),
            dma((CHUNKS,)),
            dma((CHUNKS,)),
            dma((CHUNKS,)),
            dma((CHUNKS,)),
            dma((CHUNKS,)),
            dma((CHUNKS, 4)),
        ],
        compiler_params=pltpu.CompilerParams(
            collective_id=0, has_side_effects=True, vmem_limit_bytes=56 * 1024 * 1024
        ),
    )(
        tokens, gains, jnp.swapaxes(route_ids[0], 1, 2), jnp.swapaxes(route_weights[0], 1, 2),
        picks[0, :, 0], w_gate[0, 0], w_up[0, 0], w_down[0, 0],
    )
    return out[None]


def solution(mesh):
    return jax.shard_map(
        local,
        mesh=mesh,
        in_specs=(
            P(None, "expert", None),
            P("pipe", None),
            P("pipe", None, "expert", None),
            P("pipe", None, "expert", None),
            P("pipe", None, "expert", None),
            P("pipe", "expert", None, "tensor"),
            P("pipe", "expert", None, "tensor"),
            P("pipe", "expert", "tensor", None),
        ),
        out_specs=P("pipe", None, "expert", "tensor"),
        check_vma=False,
    )
```

```python
import jax
import jax.numpy as jnp
from jax import lax
from jax.experimental import pallas as pl
from jax.experimental.pallas import tpu as pltpu
from jax.sharding import PartitionSpec as P

EPS = 1e-06
MESH = pl.DeviceIdType.MESH
BF = jnp.bfloat16
F32 = jnp.float32
CHUNKS = 4
CAP = 5
PARTS = 4


def wait_bytes(ref, sem):
    pltpu.make_async_copy(ref, ref, sem).wait()


def relay_kernel(
    tokens, gains, ids, route_w, picks, w_gate, w_up, w_down, out,
    wgu, wd, table, tables, place, comb, hin, hnew, xs, dfirst, dout, acc, squares, hid, total, relay_w,
    opp, side, relay, got, rout, ret, outbuf,
    wsem, dwsem, tsem, hsem, dsem, agsem, rssem, retsem, osem,
    s_tab, s_dw, s_tok, s_first, s_disp, s_ag, s_rs, s_ret, s_h, s_out,
):
    sec = lax.axis_index("pipe")
    rank = lax.axis_index("tensor")
    me = lax.axis_index("expert")
    last = lax.axis_size("pipe") - 1
    up1 = lax.rem(rank + 1, 4)
    dn1 = lax.rem(rank + 3, 4)
    far = lax.rem(rank + 2, 4)
    my_half = me // 4
    chip, core = me // 2, lax.rem(me, 2)
    partner = chip * 2 + 1 - core
    my_piece = core * 4 + chip

    def send(src, dst, ssem, rsem, dev):
        pltpu.make_async_remote_copy(
            src_ref=src, dst_ref=dst, send_sem=ssem, recv_sem=rsem,
            device_id=dev, device_id_type=MESH,
        ).start()

    barrier = pltpu.get_barrier_semaphore()

    def greet(dev):
        pl.semaphore_signal(barrier, inc=1, device_id=dev, device_id_type=MESH)

    for o in range(1, 8):
        greet({"expert": lax.rem(me + o, 8)})
    greet({"tensor": up1})
    greet({"tensor": dn1})
    greet({"tensor": far})

    @pl.when(sec < last)
    def _():
        for e in range(8):
            greet({"pipe": sec + 1, "expert": e})

    @pl.when(sec > 0)
    def _():
        for e in range(8):
            greet({"pipe": sec - 1, "expert": e})

    def weight_copies():
        copies = []
        for q in range(4):
            copies.append((w_gate.at[pl.ds(q * 1024, 1024), :], wgu.at[q, :, pl.ds(0, 384)]))
            copies.append((w_up.at[pl.ds(q * 1024, 1024), :], wgu.at[q, :, pl.ds(384, 384)]))
        return [pltpu.make_async_copy(a, b, wsem.at[i]) for i, (a, b) in enumerate(copies)]

    def slice_of_down(q):
        return w_down.at[:, pl.ds(pl.multiple_of(q * 1024, 128), 1024)]

    def first_down_copies():
        return [pltpu.make_async_copy(slice_of_down(q), wd.at[q], wsem.at[8 + q]) for q in range(4)]

    def own_down_copy():
        return pltpu.make_async_copy(slice_of_down(rank), wd.at[rank], wsem.at[8])

    for copy in weight_copies():
        copy.start()

    @pl.when(sec == 0)
    def _():
        for copy in first_down_copies():
            copy.start()

    @pl.when(sec > 0)
    def _():
        own_down_copy().start()

    def iota(shape, dim):
        return lax.broadcasted_iota(jnp.int32, shape, dim).astype(F32)

    def column(row, eye):
        return jnp.sum(jnp.where(eye, row, 0.0), axis=1, keepdims=True)

    sub, lane = iota((64, 64), 0), iota((64, 64), 1)
    eye = sub == lane
    shift = (lax.rem(me, 4) * 64).astype(F32)
    spread = (iota((64, 256), 0) + shift) == iota((64, 256), 1)
    row_of = iota((8, 256), 0)
    whole = jnp.zeros((8, 256), F32)
    for m in range(2):
        picked = column(picks[m : m + 1, :].astype(F32), eye)
        spot = jnp.sum(jnp.where(picked == lane, sub, 0.0), axis=0, keepdims=True)
        spot_col = column(spot, eye)
        quarter, quarter_col = jnp.floor(spot / 16.0), jnp.floor(spot_col / 16.0)
        names = [ids[m, t : t + 1, :].astype(F32) for t in range(2)]
        name_cols = [column(n, eye) for n in names]
        for t in range(2):
            slot = jnp.zeros((1, 64), F32)
            for u in range(2):
                hit = (name_cols[u] == names[t]) & (quarter_col == quarter)
                hit = hit & (spot_col * 2.0 + u < spot * 2.0 + t)
                slot = slot + jnp.sum(jnp.where(hit, 1.0, 0.0), axis=0, keepdims=True)
            at = names[t] * 80.0 + lax.rem(me, 4).astype(F32) * 20.0 + quarter * CAP + slot
            at = jnp.where(slot < CAP, at, -1.0)
            for field, value in ((t, at), (2 + t, route_w[m, t : t + 1, :])):
                placed = jnp.where(spread, column(value, eye), 0.0)
                placed = jnp.sum(placed, axis=0, keepdims=True)
                whole = whole + jnp.where(row_of == m * 4 + field, placed, 0.0)
    table[...] = whole

    greeted = 10 + jnp.where(sec < last, 8, 0) + jnp.where(sec > 0, 8, 0)
    pl.semaphore_wait(barrier, greeted)

    for o in range(1, 8):
        send(table, tables.at[0, me], s_tab.at[o - 1], tsem.at[0], {"expert": lax.rem(me + o, 8)})
    pltpu.make_async_copy(table, tables.at[0, me], tsem.at[0]).start()

    @pl.when(sec > 0)
    def _():
        for e in range(8):
            send(table, tables.at[1, me], s_tab.at[7 + e], tsem.at[1], {"pipe": sec - 1, "expert": e})

    @pl.when(sec == 0)
    def _():
        start = pl.multiple_of(rank * 1024, 128)
        row = pl.multiple_of(lax.rem(me, 4) * 64, 64)
        for m in range(2):
            k = m * 2 + my_half
            for o in range(1, 8):
                j = lax.rem(me + o, 8)
                send(
                    tokens.at[m, :, pl.ds(pl.multiple_of(start + j * 128, 128), 128)],
                    hin.at[k, pl.ds(row, 64), :],
                    s_tok.at[m, o - 1], hsem.at[k], {"expert": j},
                )
            pltpu.make_async_copy(
                tokens.at[m, :, pl.ds(pl.multiple_of(start + me * 128, 128), 128)],
                hin.at[k, pl.ds(row, 64), :], hsem.at[k],
            ).start()

    to_up, to_dn = {"tensor": up1}, {"tensor": dn1}
    top, rest = pl.ds(0, 192), pl.ds(192, 192)

    @pl.when(sec > 0)
    def _():
        distant = pl.ds(pl.multiple_of(far * 1024, 128), 1024)
        send(w_down.at[top, distant], relay_w.at[0], s_dw.at[0], dwsem.at[2], to_up)
        send(w_down.at[rest, distant], relay_w.at[1], s_dw.at[1], dwsem.at[3], to_dn)
        send(slice_of_down(up1), wd.at[rank], s_dw.at[2], dwsem.at[0], to_up)
        send(slice_of_down(dn1), wd.at[rank], s_dw.at[3], dwsem.at[1], to_dn)
        wait_bytes(relay_w.at[0], dwsem.at[2])
        send(relay_w.at[0], wd.at[dn1, top], s_dw.at[4], dwsem.at[4], to_up)
        wait_bytes(relay_w.at[1], dwsem.at[3])
        send(relay_w.at[1], wd.at[up1, rest], s_dw.at[5], dwsem.at[5], to_dn)

    slot_rows = iota((640, 256), 0)
    slot_cols = iota((256, 640), 1)
    eye256 = iota((256, 256), 0) == iota((256, 256), 1)

    def fields(which, k, names):
        m, half = k // 2, lax.rem(k, 2)
        rows = []
        for f in names:
            at = pl.ds(m * 4 + f, 1)
            row = tables[which, half * 4, at, :]
            for i in range(1, 4):
                row = row + tables[which, half * 4 + i, at, :]
            rows.append(row)
        return rows

    def placing(which, k):
        a, b = fields(which, k, (0, 1))
        return jnp.where((slot_rows == a) | (slot_rows == b), 1.0, 0.0).astype(BF)

    def place_rows(matrix, rows, dest, k):
        moved = jnp.dot(matrix, rows, preferred_element_type=F32).astype(BF)
        for e in range(8):
            dest[k, e] = moved[e * 80 : (e + 1) * 80]

    def far_first(side):
        order = [lax.rem(chip + o, 4) * 2 for o in (2, side, 4 - side)]
        return [base + c for base in order for c in range(2)]

    def first(k):
        place_rows(placing(0, k), hin[k], dfirst, k)
        for o in range(1, 8):
            e = lax.rem(me + o, 8)
            send(dfirst.at[k, e], xs.at[k, 0, my_piece], s_first.at[k], dsem.at[k, my_piece], {"expert": e})
        pltpu.make_async_copy(dfirst.at[k, me], xs.at[k, 0, my_piece], dsem.at[k, my_piece]).start()

    @pl.when(sec == 0)
    def _():
        wait_bytes(tables.at[0], tsem.at[0])
        wait_bytes(hin.at[0], hsem.at[0])
        first(0)

    def prepare(k):
        @pl.when((k < CHUNKS - 1) & (sec == 0))
        def _():
            wait_bytes(hin.at[k + 1], hsem.at[k + 1])
            first(k + 1)

        @pl.when((k == 0) & (sec > 0))
        def _():
            wait_bytes(tables.at[0], tsem.at[0])

        @pl.when((k == 0) & (sec < last))
        def _():
            wait_bytes(tables.at[1], tsem.at[1])

        cols = [column(row, eye256) for row in fields(0, k, (0, 1, 2, 3))]
        mix = jnp.where(slot_cols == cols[0], cols[2], 0.0)
        mix = mix + jnp.where(slot_cols == cols[1], cols[3], 0.0)
        high = mix.astype(BF)
        comb[k, 0] = high
        comb[k, 1] = (mix - high.astype(F32)).astype(BF)

        @pl.when(sec < last)
        def _():
            place[k] = placing(1, k)

        @pl.when(k == 0)
        def _():
            for copy in weight_copies():
                copy.wait()

        @pl.when((k == 0) & (sec == 0))
        def _():
            for copy in first_down_copies():
                copy.wait()

        @pl.when((k == 0) & (sec > 0))
        def _():
            own_down_copy().wait()
            wait_bytes(wd.at[dn1], dwsem.at[0])
            wait_bytes(wd.at[up1], dwsem.at[1])
            wait_bytes(wd.at[far, top], dwsem.at[4])
            wait_bytes(wd.at[far, rest], dwsem.at[5])

    lo, hi = pl.ds(0, 4), pl.ds(4, 4)

    def lanes(value, j):
        return value[:, j * 128 : (j + 1) * 128]

    def part(k, rel, origin):
        x = jnp.concatenate([xs[k, rel, (j % 2) * 4 + j // 2] for j in range(8)], axis=1).astype(F32)
        scaled = x * gains[:, pl.ds(pl.multiple_of(origin * 1024, 128), 1024)]
        both = jnp.dot(scaled.astype(BF), wgu[origin], preferred_element_type=F32)
        return jnp.sum(x * x, axis=1, keepdims=True), both

    def chips():
        return [lax.rem(chip + o, 4) for o in (0, 1, 3, 2)]

    def low(p):
        return pl.ds(p, 1)

    def high_of(p):
        return pl.ds(4 + p, 1)

    def gather_start(k):
        ssem = s_ag.at[k]
        for p in chips():
            wait_bytes(xs.at[k, 0, low(p)], dsem.at[k, p])
            send(xs.at[k, 0, low(p)], xs.at[k, 1, low(p)], ssem, agsem.at[k, p], to_up)
            wait_bytes(xs.at[k, 0, high_of(p)], dsem.at[k, PARTS + p])
            send(xs.at[k, 0, high_of(p)], xs.at[k, 2, high_of(p)], ssem, agsem.at[k, PARTS + p], to_dn)
        send(xs.at[k, 0, lo], xs.at[k, 2, lo], ssem, agsem.at[k, 4 * PARTS], to_dn)
        send(xs.at[k, 0, hi], xs.at[k, 1, hi], ssem, agsem.at[k, 4 * PARTS + 1], to_up)

    def gather_relay(k):
        ssem = s_ag.at[k]
        sq, both = part(k, 0, rank)
        acc[...] = both
        squares[...] = jnp.broadcast_to(sq, (80, 128))
        for p in chips():
            wait_bytes(xs.at[k, 1, low(p)], agsem.at[k, p])
            send(xs.at[k, 1, low(p)], xs.at[k, 3, low(p)], ssem, agsem.at[k, 2 * PARTS + p], to_up)
            wait_bytes(xs.at[k, 2, high_of(p)], agsem.at[k, PARTS + p])
            send(xs.at[k, 2, high_of(p)], xs.at[k, 3, high_of(p)], ssem, agsem.at[k, 3 * PARTS + p], to_dn)

    def feed_forward(k):
        both, sq = acc[...], squares[:, 0:1]
        wait_bytes(xs.at[k, 1, hi], agsem.at[k, 4 * PARTS + 1])
        s, b = part(k, 1, dn1)
        sq, both = sq + s, both + b
        wait_bytes(xs.at[k, 2, lo], agsem.at[k, 4 * PARTS])
        s, b = part(k, 2, up1)
        sq, both = sq + s, both + b
        for p in range(PARTS):
            wait_bytes(xs.at[k, 3, low(p)], agsem.at[k, 2 * PARTS + p])
            wait_bytes(xs.at[k, 3, high_of(p)], agsem.at[k, 3 * PARTS + p])
        s, b = part(k, 3, far)
        sq, both = sq + s, both + b
        both = both * lax.rsqrt(sq * (1.0 / 4096.0) + EPS)
        gate, up = both[:, :384], both[:, 384:]
        hid[k, 0] = (gate / (1.0 + jnp.exp(-gate)) * up).astype(BF)

    def down(k, q):
        return jnp.dot(hid[k, 0], wd[q], preferred_element_type=F32).astype(BF)

    def spread_start(k):
        ssem = s_rs.at[k]
        send(hid.at[k, 0], hid.at[k, 3], ssem, rssem.at[k, 2], {"tensor": far})
        send(hid.at[k, 0], hid.at[k, 1], ssem, rssem.at[k, 0], to_up)
        send(hid.at[k, 0], hid.at[k, 2], ssem, rssem.at[k, 1], to_dn)
        total[...] = jnp.dot(hid[k, 0], wd[rank], preferred_element_type=F32)

    def spread_end(k):
        wait_bytes(hid.at[k, 1], rssem.at[k, 0])
        total[...] += jnp.dot(hid[k, 1], wd[dn1], preferred_element_type=F32)
        wait_bytes(hid.at[k, 2], rssem.at[k, 1])
        total[...] += jnp.dot(hid[k, 2], wd[up1], preferred_element_type=F32)
        wait_bytes(hid.at[k, 3], rssem.at[k, 2])
        done = (total[...] + jnp.dot(hid[k, 3], wd[far], preferred_element_type=F32)).astype(BF)
        for j in range(8):
            rout[k, j] = lanes(done, j)
        for j in far_first(1):
            send(rout.at[k, j], ret.at[k, me], s_ret.at[k], retsem.at[k], {"expert": j})
        send(rout.at[k, partner], ret.at[k, me], s_ret.at[k], retsem.at[k], {"expert": partner})
        pltpu.make_async_copy(rout.at[k, me], ret.at[k, me], retsem.at[k]).start()

    def first_layer_sum_start(k):
        ssem = s_rs.at[k]
        value = down(k, far)
        for j in range(8):
            opp[k, j] = lanes(value, j)
        for p in range(PARTS):
            send(opp.at[k, low(p)], relay.at[k, 0, low(p)], ssem, rssem.at[k, p], to_up)
            send(opp.at[k, high_of(p)], relay.at[k, 1, low(p)], ssem, rssem.at[k, PARTS + p], to_dn)
        value = down(k, up1)
        for j in range(8):
            side[k, 0, j] = lanes(value, j)
        send(side.at[k, 0, hi], got.at[k, 0, hi], ssem, rssem.at[k, 4 * PARTS], to_up)
        value = down(k, dn1)
        for j in range(8):
            side[k, 1, j] = lanes(value, j)
        send(side.at[k, 1, lo], got.at[k, 1, lo], ssem, rssem.at[k, 4 * PARTS + 1], to_dn)
        value = down(k, rank)
        for j in range(8):
            rout[k, j] = lanes(value, j)

    def first_layer_sum_relay(k):
        ssem = s_rs.at[k]
        for p in range(PARTS):
            wait_bytes(relay.at[k, 0, low(p)], rssem.at[k, p])
            for j in range(p, p + 1):
                side[k, 0, j] = (side[k, 0, j].astype(F32) + relay[k, 0, j].astype(F32)).astype(BF)
            send(side.at[k, 0, low(p)], got.at[k, 0, low(p)], ssem, rssem.at[k, 2 * PARTS + p], to_up)
            wait_bytes(relay.at[k, 1, low(p)], rssem.at[k, PARTS + p])
            for j in range(p, p + 1):
                side[k, 1, 4 + j] = (side[k, 1, 4 + j].astype(F32) + relay[k, 1, j].astype(F32)).astype(BF)
            send(side.at[k, 1, high_of(p)], got.at[k, 1, high_of(p)], ssem, rssem.at[k, 3 * PARTS + p], to_dn)

    def give_back(k, j):
        total = rout[k, j].astype(F32) + got[k, 0, j].astype(F32) + got[k, 1, j].astype(F32)
        rout[k, j] = total.astype(BF)

    def ship(k, j):
        @pl.when(me == j)
        def _():
            pltpu.make_async_copy(rout.at[k, j], ret.at[k, me], retsem.at[k]).start()

        @pl.when(me != j)
        def _():
            send(rout.at[k, j], ret.at[k, me], s_ret.at[k], retsem.at[k], {"expert": j})

    def first_layer_sum_end(k):
        wait_bytes(got.at[k, 1, lo], rssem.at[k, 4 * PARTS + 1])
        wait_bytes(got.at[k, 0, hi], rssem.at[k, 4 * PARTS])
        for p in range(PARTS):
            for which in (0, 1):
                j = 4 * which + p
                wait_bytes(got.at[k, which, pl.ds(j, 1)], rssem.at[k, (2 + which) * PARTS + p])
                give_back(k, j)
                ship(k, j)

    def sum_start(k):
        @pl.when(sec == 0)
        def _():
            first_layer_sum_start(k)

        @pl.when(sec > 0)
        def _():
            spread_start(k)

    def sum_relay(k):
        @pl.when(sec == 0)
        def _():
            first_layer_sum_relay(k)

    def sum_end(k):
        @pl.when(sec == 0)
        def _():
            first_layer_sum_end(k)

        @pl.when(sec > 0)
        def _():
            spread_end(k)

    def publish(k):
        m, half = k // 2, lax.rem(k, 2)
        mine = pl.ds(pl.multiple_of(me * 128, 128), 128)
        for i in range(4):
            owner = half * 4 + i
            block = hnew.at[k, pl.ds(i * 64, 64), :]
            place_at = outbuf.at[m, :, mine]

            @pl.when(owner == me)
            def _():
                pltpu.make_async_copy(block, place_at, osem).start()

            @pl.when(owner != me)
            def _():
                send(block, place_at, s_out.at[k, i], osem, {"expert": owner})

    def home(k):
        @pl.when(sec > 0)
        def _():
            wait_bytes(hin.at[k], hsem.at[k])

        wait_bytes(ret.at[k], retsem.at[k])
        back = ret[k].reshape(640, 128)
        update = jnp.dot(comb[k, 0], back, preferred_element_type=F32)
        update = update + jnp.dot(comb[k, 1], back, preferred_element_type=F32)
        fresh = (hin[k].astype(F32) + update).astype(BF)

        @pl.when(sec < last)
        def _():
            place_rows(place[k], fresh, dout, k)
            for e in far_first(1 + 2 * lax.rem(sec, 2)) + [chip * 2, chip * 2 + 1]:
                send(
                    dout.at[k, e], xs.at[k, 0, my_piece], s_disp.at[k], dsem.at[k, my_piece],
                    {"pipe": sec + 1, "expert": e},
                )

        hnew[k] = fresh

        @pl.when(sec < last)
        def _():
            send(hnew.at[k], hin.at[k], s_h.at[k], hsem.at[k], {"pipe": sec + 1})

        @pl.when(sec == last)
        def _():
            publish(k)

    @pl.when(sec == 0)
    def _():
        def turn(k, carry):
            @pl.when((k < CHUNKS))
            def _():
                gather_start(k)
                prepare(k)

            @pl.when((k >= 1))
            def _():
                sum_end(k - 1)

            @pl.when((k < CHUNKS))
            def _():
                gather_relay(k)
                feed_forward(k)

            @pl.when((k >= 1))
            def _():
                home(k - 1)

            @pl.when((k < CHUNKS))
            def _():
                sum_start(k)
                sum_relay(k)

            return carry

        lax.fori_loop(0, CHUNKS + 1, turn, 0)

    @pl.when(sec > 0)
    def _():
        def turn(k, carry):
            @pl.when((k < CHUNKS))
            def _():
                gather_start(k)
                prepare(k)
                gather_relay(k)

            @pl.when((k >= 1))
            def _():
                home(k - 1)

            @pl.when((k < CHUNKS))
            def _():
                feed_forward(k)
                sum_start(k)
                sum_relay(k)
                sum_end(k)

            return carry

        lax.fori_loop(0, CHUNKS + 1, turn, 0)

    @pl.when(sec < last)
    def _():
        lax.fori_loop(0, CHUNKS, lambda k, carry: (publish(k), carry)[1], 0)

    for o in range(7):
        wait_bytes(table, s_tab.at[o])

    @pl.when(sec > 0)
    def _():
        for e in range(8):
            wait_bytes(table, s_tab.at[7 + e])
        for i in range(4):
            wait_bytes(relay_w.at[0] if i < 2 else wd.at[0], s_dw.at[i])
        for i in range(2):
            wait_bytes(relay_w.at[i], s_dw.at[4 + i])

    @pl.when(sec == 0)
    def _():
        for m in range(2):
            for o in range(7):
                wait_bytes(hin.at[m, pl.ds(0, 64), :], s_tok.at[m, o])
        for k in range(CHUNKS):
            wait_bytes(dfirst.at[k, pl.ds(0, 7)], s_first.at[k])

    def drain(k, carry):
        wait_bytes(xs.at[k, pl.ds(0, 3)], s_ag.at[k])

        @pl.when(sec == 0)
        def _():
            wait_bytes(xs.at[k, pl.ds(0, 3)], s_rs.at[k])

        @pl.when(sec > 0)
        def _():
            wait_bytes(hid.at[k, pl.ds(0, 3)], s_rs.at[k])

        wait_bytes(ret.at[k, pl.ds(0, 7)], s_ret.at[k])

        @pl.when(sec < last)
        def _():
            wait_bytes(dout.at[k], s_disp.at[k])
            wait_bytes(hnew.at[k], s_h.at[k])

        for i in range(4):
            owner = lax.rem(k, 2) * 4 + i

            @pl.when(owner != me)
            def _():
                wait_bytes(hnew.at[k, pl.ds(i * 64, 64), :], s_out.at[k, i])

        return carry

    lax.fori_loop(0, CHUNKS, drain, 0)
    wait_bytes(outbuf, osem)
    final = pltpu.make_async_copy(outbuf, out, wsem.at[0])
    final.start()
    final.wait()


def local(tokens, gains, route_ids, route_weights, picks, w_gate, w_up, w_down):
    vmem = pl.BlockSpec(memory_space=pltpu.VMEM)
    anywhere = pl.BlockSpec(memory_space=pl.ANY)
    dma = pltpu.SemaphoreType.DMA
    out = pl.pallas_call(
        relay_kernel,
        name="relay",
        out_shape=jax.ShapeDtypeStruct((2, 64, 1024), BF),
        in_specs=[anywhere, vmem, vmem, vmem, vmem, anywhere, anywhere, anywhere],
        out_specs=anywhere,
        scratch_shapes=[
            pltpu.VMEM((4, 1024, 768), BF),
            pltpu.VMEM((4, 384, 1024), BF),
            pltpu.VMEM((8, 256), F32),
            pltpu.VMEM((2, 8, 8, 256), F32),
            pltpu.VMEM((CHUNKS, 640, 256), BF),
            pltpu.VMEM((CHUNKS, 2, 256, 640), BF),
            pltpu.VMEM((CHUNKS, 256, 128), BF),
            pltpu.VMEM((CHUNKS, 256, 128), BF),
            pltpu.VMEM((CHUNKS, 4, 8, 80, 128), BF),
            pltpu.VMEM((CHUNKS, 8, 80, 128), BF),
            pltpu.VMEM((CHUNKS, 8, 80, 128), BF),
            pltpu.VMEM((80, 768), F32),
            pltpu.VMEM((80, 128), F32),
            pltpu.VMEM((CHUNKS, 4, 80, 384), BF),
            pltpu.VMEM((80, 1024), F32),
            pltpu.VMEM((2, 192, 1024), BF),
            pltpu.VMEM((CHUNKS, 8, 80, 128), BF),
            pltpu.VMEM((CHUNKS, 2, 8, 80, 128), BF),
            pltpu.VMEM((CHUNKS, 2, 4, 80, 128), BF),
            pltpu.VMEM((CHUNKS, 2, 8, 80, 128), BF),
            pltpu.VMEM((CHUNKS, 8, 80, 128), BF),
            pltpu.VMEM((CHUNKS, 8, 80, 128), BF),
            pltpu.VMEM((2, 64, 1024), BF),
            dma((12,)),
            dma((6,)),
            dma((2,)),
            dma((CHUNKS,)),
            dma((CHUNKS, 2 * PARTS)),
            dma((CHUNKS, 4 * PARTS + 2)),
            dma((CHUNKS, 4 * PARTS + 2)),
            dma((CHUNKS,)),
            dma(()),
            dma((15,)),
            dma((6,)),
            dma((2, 7)),
            dma((CHUNKS,)),
            dma((CHUNKS,)),
            dma((CHUNKS,)),
            dma((CHUNKS,)),
            dma((CHUNKS,)),
            dma((CHUNKS,)),
            dma((CHUNKS, 4)),
        ],
        compiler_params=pltpu.CompilerParams(
            collective_id=0, has_side_effects=True, vmem_limit_bytes=56 * 1024 * 1024
        ),
    )(
        tokens, gains, jnp.swapaxes(route_ids[0], 1, 2), jnp.swapaxes(route_weights[0], 1, 2),
        picks[0, :, 0], w_gate[0, 0], w_up[0, 0], w_down[0, 0],
    )
    return out[None]


def solution(mesh):
    return jax.shard_map(
        local,
        mesh=mesh,
        in_specs=(
            P(None, "expert", None),
            P("pipe", None),
            P("pipe", None, "expert", None),
            P("pipe", None, "expert", None),
            P("pipe", None, "expert", None),
            P("pipe", "expert", None, "tensor"),
            P("pipe", "expert", None, "tensor"),
            P("pipe", "expert", "tensor", None),
        ),
        out_specs=P("pipe", None, "expert", "tensor"),
        check_vma=False,
    )
```

```python
import jax
import jax.numpy as jnp
from jax import lax
from jax.experimental import pallas as pl
from jax.experimental.pallas import tpu as pltpu
from jax.sharding import PartitionSpec as P

EPS = 1e-06
MESH = pl.DeviceIdType.MESH
BF = jnp.bfloat16
F32 = jnp.float32
CHUNKS = 4
CAP = 5
PARTS = 4


def wait_bytes(ref, sem):
    pltpu.make_async_copy(ref, ref, sem).wait()


def relay_kernel(
    tokens, gains, ids, route_w, picks, w_gate, w_up, w_down, out,
    wgu, wd, table, tables, place, comb, hin, hnew, xs, dfirst, dout, acc, squares, hid, total, relay_w,
    opp, side, relay, got, rout, ret, outbuf,
    wsem, dwsem, tsem, hsem, dsem, agsem, rssem, retsem, osem,
    s_tab, s_dw, s_tok, s_first, s_disp, s_ag, s_rs, s_ret, s_h, s_out,
):
    sec = lax.axis_index("pipe")
    rank = lax.axis_index("tensor")
    me = lax.axis_index("expert")
    last = lax.axis_size("pipe") - 1
    up1 = lax.rem(rank + 1, 4)
    dn1 = lax.rem(rank + 3, 4)
    far = lax.rem(rank + 2, 4)
    my_half = me // 4
    chip, core = me // 2, lax.rem(me, 2)
    partner = chip * 2 + 1 - core
    my_piece = core * 4 + chip

    def send(src, dst, ssem, rsem, dev):
        pltpu.make_async_remote_copy(
            src_ref=src, dst_ref=dst, send_sem=ssem, recv_sem=rsem,
            device_id=dev, device_id_type=MESH,
        ).start()

    barrier = pltpu.get_barrier_semaphore()

    def greet(dev):
        pl.semaphore_signal(barrier, inc=1, device_id=dev, device_id_type=MESH)

    for o in range(1, 8):
        greet({"expert": lax.rem(me + o, 8)})
    greet({"tensor": up1})
    greet({"tensor": dn1})
    greet({"tensor": far})

    @pl.when(sec < last)
    def _():
        for e in range(8):
            greet({"pipe": sec + 1, "expert": e})

    @pl.when(sec > 0)
    def _():
        for e in range(8):
            greet({"pipe": sec - 1, "expert": e})

    def weight_copies():
        copies = []
        for q in range(4):
            copies.append((w_gate.at[pl.ds(q * 1024, 1024), :], wgu.at[q, :, pl.ds(0, 384)]))
            copies.append((w_up.at[pl.ds(q * 1024, 1024), :], wgu.at[q, :, pl.ds(384, 384)]))
        return [pltpu.make_async_copy(a, b, wsem.at[i]) for i, (a, b) in enumerate(copies)]

    def slice_of_down(q):
        return w_down.at[:, pl.ds(pl.multiple_of(q * 1024, 128), 1024)]

    def first_down_copies():
        return [pltpu.make_async_copy(slice_of_down(q), wd.at[q], wsem.at[8 + q]) for q in range(4)]

    def own_down_copy():
        return pltpu.make_async_copy(slice_of_down(rank), wd.at[rank], wsem.at[8])

    for copy in weight_copies():
        copy.start()

    @pl.when(sec == 0)
    def _():
        for copy in first_down_copies():
            copy.start()

    @pl.when(sec > 0)
    def _():
        own_down_copy().start()

    def iota(shape, dim):
        return lax.broadcasted_iota(jnp.int32, shape, dim).astype(F32)

    def column(row, eye):
        return jnp.sum(jnp.where(eye, row, 0.0), axis=1, keepdims=True)

    sub, lane = iota((64, 64), 0), iota((64, 64), 1)
    eye = sub == lane
    shift = (lax.rem(me, 4) * 64).astype(F32)
    spread = (iota((64, 256), 0) + shift) == iota((64, 256), 1)
    row_of = iota((8, 256), 0)
    whole = jnp.zeros((8, 256), F32)
    for m in range(2):
        picked = column(picks[m : m + 1, :].astype(F32), eye)
        spot = jnp.sum(jnp.where(picked == lane, sub, 0.0), axis=0, keepdims=True)
        spot_col = column(spot, eye)
        quarter, quarter_col = jnp.floor(spot / 16.0), jnp.floor(spot_col / 16.0)
        names = [ids[m, t : t + 1, :].astype(F32) for t in range(2)]
        name_cols = [column(n, eye) for n in names]
        for t in range(2):
            slot = jnp.zeros((1, 64), F32)
            for u in range(2):
                hit = (name_cols[u] == names[t]) & (quarter_col == quarter)
                hit = hit & (spot_col * 2.0 + u < spot * 2.0 + t)
                slot = slot + jnp.sum(jnp.where(hit, 1.0, 0.0), axis=0, keepdims=True)
            at = names[t] * 80.0 + lax.rem(me, 4).astype(F32) * 20.0 + quarter * CAP + slot
            at = jnp.where(slot < CAP, at, -1.0)
            for field, value in ((t, at), (2 + t, route_w[m, t : t + 1, :])):
                placed = jnp.where(spread, column(value, eye), 0.0)
                placed = jnp.sum(placed, axis=0, keepdims=True)
                whole = whole + jnp.where(row_of == m * 4 + field, placed, 0.0)
    table[...] = whole

    greeted = 10 + jnp.where(sec < last, 8, 0) + jnp.where(sec > 0, 8, 0)
    pl.semaphore_wait(barrier, greeted)

    for o in range(1, 8):
        send(table, tables.at[0, me], s_tab.at[o - 1], tsem.at[0], {"expert": lax.rem(me + o, 8)})
    pltpu.make_async_copy(table, tables.at[0, me], tsem.at[0]).start()

    @pl.when(sec > 0)
    def _():
        for e in range(8):
            send(table, tables.at[1, me], s_tab.at[7 + e], tsem.at[1], {"pipe": sec - 1, "expert": e})

    @pl.when(sec == 0)
    def _():
        start = pl.multiple_of(rank * 1024, 128)
        row = pl.multiple_of(lax.rem(me, 4) * 64, 64)
        for m in range(2):
            k = m * 2 + my_half
            for o in range(1, 8):
                j = lax.rem(me + o, 8)
                send(
                    tokens.at[m, :, pl.ds(pl.multiple_of(start + j * 128, 128), 128)],
                    hin.at[k, pl.ds(row, 64), :],
                    s_tok.at[m, o - 1], hsem.at[k], {"expert": j},
                )
            pltpu.make_async_copy(
                tokens.at[m, :, pl.ds(pl.multiple_of(start + me * 128, 128), 128)],
                hin.at[k, pl.ds(row, 64), :], hsem.at[k],
            ).start()

    to_up, to_dn = {"tensor": up1}, {"tensor": dn1}
    top, rest = pl.ds(0, 192), pl.ds(192, 192)

    @pl.when(sec > 0)
    def _():
        distant = pl.ds(pl.multiple_of(far * 1024, 128), 1024)
        send(w_down.at[top, distant], relay_w.at[0], s_dw.at[0], dwsem.at[2], to_up)
        send(w_down.at[rest, distant], relay_w.at[1], s_dw.at[1], dwsem.at[3], to_dn)
        send(slice_of_down(up1), wd.at[rank], s_dw.at[2], dwsem.at[0], to_up)
        send(slice_of_down(dn1), wd.at[rank], s_dw.at[3], dwsem.at[1], to_dn)
        wait_bytes(relay_w.at[0], dwsem.at[2])
        send(relay_w.at[0], wd.at[dn1, top], s_dw.at[4], dwsem.at[4], to_up)
        wait_bytes(relay_w.at[1], dwsem.at[3])
        send(relay_w.at[1], wd.at[up1, rest], s_dw.at[5], dwsem.at[5], to_dn)

    slot_rows = iota((640, 256), 0)
    slot_cols = iota((256, 640), 1)
    eye256 = iota((256, 256), 0) == iota((256, 256), 1)

    def fields(which, k, names):
        m, half = k // 2, lax.rem(k, 2)
        rows = []
        for f in names:
            at = pl.ds(m * 4 + f, 1)
            row = tables[which, half * 4, at, :]
            for i in range(1, 4):
                row = row + tables[which, half * 4 + i, at, :]
            rows.append(row)
        return rows

    def placing(which, k):
        a, b = fields(which, k, (0, 1))
        return jnp.where((slot_rows == a) | (slot_rows == b), 1.0, 0.0).astype(BF)

    def place_rows(matrix, rows, dest, k):
        moved = jnp.dot(matrix, rows, preferred_element_type=F32).astype(BF)
        for e in range(8):
            dest[k, e] = moved[e * 80 : (e + 1) * 80]

    def far_first(side):
        order = [lax.rem(chip + o, 4) * 2 for o in (2, side, 4 - side)]
        return [base + c for base in order for c in range(2)]

    def first(k):
        place_rows(placing(0, k), hin[k], dfirst, k)
        for o in range(1, 8):
            e = lax.rem(me + o, 8)
            send(dfirst.at[k, e], xs.at[k, 0, my_piece], s_first.at[k], dsem.at[k, my_piece], {"expert": e})
        pltpu.make_async_copy(dfirst.at[k, me], xs.at[k, 0, my_piece], dsem.at[k, my_piece]).start()

    @pl.when(sec == 0)
    def _():
        wait_bytes(tables.at[0], tsem.at[0])
        wait_bytes(hin.at[0], hsem.at[0])
        first(0)

    def prepare(k):
        @pl.when((k < CHUNKS - 1) & (sec == 0))
        def _():
            wait_bytes(hin.at[k + 1], hsem.at[k + 1])
            first(k + 1)

        @pl.when((k == 0) & (sec > 0))
        def _():
            wait_bytes(tables.at[0], tsem.at[0])

        @pl.when((k == 0) & (sec < last))
        def _():
            wait_bytes(tables.at[1], tsem.at[1])

        cols = [column(row, eye256) for row in fields(0, k, (0, 1, 2, 3))]
        mix = jnp.where(slot_cols == cols[0], cols[2], 0.0)
        mix = mix + jnp.where(slot_cols == cols[1], cols[3], 0.0)
        high = mix.astype(BF)
        comb[k, 0] = high
        comb[k, 1] = (mix - high.astype(F32)).astype(BF)

        @pl.when(sec < last)
        def _():
            place[k] = placing(1, k)

        @pl.when(k == 0)
        def _():
            for copy in weight_copies():
                copy.wait()

        @pl.when((k == 0) & (sec == 0))
        def _():
            for copy in first_down_copies():
                copy.wait()

        @pl.when((k == 0) & (sec > 0))
        def _():
            own_down_copy().wait()
            wait_bytes(wd.at[dn1], dwsem.at[0])
            wait_bytes(wd.at[up1], dwsem.at[1])
            wait_bytes(wd.at[far, top], dwsem.at[4])
            wait_bytes(wd.at[far, rest], dwsem.at[5])

    lo, hi = pl.ds(0, 4), pl.ds(4, 4)

    def lanes(value, j):
        return value[:, j * 128 : (j + 1) * 128]

    def part(k, rel, origin):
        x = jnp.concatenate([xs[k, rel, (j % 2) * 4 + j // 2] for j in range(8)], axis=1).astype(F32)
        scaled = x * gains[:, pl.ds(pl.multiple_of(origin * 1024, 128), 1024)]
        both = jnp.dot(scaled.astype(BF), wgu[origin], preferred_element_type=F32)
        return jnp.sum(x * x, axis=1, keepdims=True), both

    def chips():
        return [lax.rem(chip + o, 4) for o in (0, 1, 3, 2)]

    def low(p):
        return pl.ds(p, 1)

    def high_of(p):
        return pl.ds(4 + p, 1)

    def gather_start(k):
        ssem = s_ag.at[k]
        for p in chips():
            wait_bytes(xs.at[k, 0, low(p)], dsem.at[k, p])
            send(xs.at[k, 0, low(p)], xs.at[k, 1, low(p)], ssem, agsem.at[k, p], to_up)
            wait_bytes(xs.at[k, 0, high_of(p)], dsem.at[k, PARTS + p])
            send(xs.at[k, 0, high_of(p)], xs.at[k, 2, high_of(p)], ssem, agsem.at[k, PARTS + p], to_dn)
        send(xs.at[k, 0, lo], xs.at[k, 2, lo], ssem, agsem.at[k, 4 * PARTS], to_dn)
        send(xs.at[k, 0, hi], xs.at[k, 1, hi], ssem, agsem.at[k, 4 * PARTS + 1], to_up)

    def gather_relay(k):
        ssem = s_ag.at[k]
        sq, both = part(k, 0, rank)
        acc[...] = both
        squares[...] = jnp.broadcast_to(sq, (80, 128))
        for p in chips():
            wait_bytes(xs.at[k, 1, low(p)], agsem.at[k, p])
            send(xs.at[k, 1, low(p)], xs.at[k, 3, low(p)], ssem, agsem.at[k, 2 * PARTS + p], to_up)
            wait_bytes(xs.at[k, 2, high_of(p)], agsem.at[k, PARTS + p])
            send(xs.at[k, 2, high_of(p)], xs.at[k, 3, high_of(p)], ssem, agsem.at[k, 3 * PARTS + p], to_dn)

    def feed_forward(k):
        both, sq = acc[...], squares[:, 0:1]
        wait_bytes(xs.at[k, 1, hi], agsem.at[k, 4 * PARTS + 1])
        s, b = part(k, 1, dn1)
        sq, both = sq + s, both + b
        wait_bytes(xs.at[k, 2, lo], agsem.at[k, 4 * PARTS])
        s, b = part(k, 2, up1)
        sq, both = sq + s, both + b
        for p in range(PARTS):
            wait_bytes(xs.at[k, 3, low(p)], agsem.at[k, 2 * PARTS + p])
            wait_bytes(xs.at[k, 3, high_of(p)], agsem.at[k, 3 * PARTS + p])
        s, b = part(k, 3, far)
        sq, both = sq + s, both + b
        both = both * lax.rsqrt(sq * (1.0 / 4096.0) + EPS)
        gate, up = both[:, :384], both[:, 384:]
        hid[k, 0] = (gate / (1.0 + jnp.exp(-gate)) * up).astype(BF)

    def down(k, q):
        return jnp.dot(hid[k, 0], wd[q], preferred_element_type=F32).astype(BF)

    def spread_start(k):
        ssem = s_rs.at[k]
        send(hid.at[k, 0], hid.at[k, 3], ssem, rssem.at[k, 2], {"tensor": far})
        send(hid.at[k, 0], hid.at[k, 1], ssem, rssem.at[k, 0], to_up)
        send(hid.at[k, 0], hid.at[k, 2], ssem, rssem.at[k, 1], to_dn)
        total[...] = jnp.dot(hid[k, 0], wd[rank], preferred_element_type=F32)

    def spread_end(k):
        wait_bytes(hid.at[k, 1], rssem.at[k, 0])
        total[...] += jnp.dot(hid[k, 1], wd[dn1], preferred_element_type=F32)
        wait_bytes(hid.at[k, 2], rssem.at[k, 1])
        total[...] += jnp.dot(hid[k, 2], wd[up1], preferred_element_type=F32)
        wait_bytes(hid.at[k, 3], rssem.at[k, 2])
        done = (total[...] + jnp.dot(hid[k, 3], wd[far], preferred_element_type=F32)).astype(BF)
        for j in range(8):
            rout[k, j] = lanes(done, j)
        for j in far_first(1):
            send(rout.at[k, j], ret.at[k, me], s_ret.at[k], retsem.at[k], {"expert": j})
        send(rout.at[k, partner], ret.at[k, me], s_ret.at[k], retsem.at[k], {"expert": partner})
        pltpu.make_async_copy(rout.at[k, me], ret.at[k, me], retsem.at[k]).start()

    def first_layer_sum_start(k):
        ssem = s_rs.at[k]
        value = down(k, far)
        for j in range(8):
            opp[k, j] = lanes(value, j)
        for p in range(PARTS):
            send(opp.at[k, low(p)], relay.at[k, 0, low(p)], ssem, rssem.at[k, p], to_up)
            send(opp.at[k, high_of(p)], relay.at[k, 1, low(p)], ssem, rssem.at[k, PARTS + p], to_dn)
        value = down(k, up1)
        for j in range(8):
            side[k, 0, j] = lanes(value, j)
        send(side.at[k, 0, hi], got.at[k, 0, hi], ssem, rssem.at[k, 4 * PARTS], to_up)
        value = down(k, dn1)
        for j in range(8):
            side[k, 1, j] = lanes(value, j)
        send(side.at[k, 1, lo], got.at[k, 1, lo], ssem, rssem.at[k, 4 * PARTS + 1], to_dn)
        value = down(k, rank)
        for j in range(8):
            rout[k, j] = lanes(value, j)

    def first_layer_sum_relay(k):
        ssem = s_rs.at[k]
        for p in range(PARTS):
            wait_bytes(relay.at[k, 0, low(p)], rssem.at[k, p])
            for j in range(p, p + 1):
                side[k, 0, j] = (side[k, 0, j].astype(F32) + relay[k, 0, j].astype(F32)).astype(BF)
            send(side.at[k, 0, low(p)], got.at[k, 0, low(p)], ssem, rssem.at[k, 2 * PARTS + p], to_up)
            wait_bytes(relay.at[k, 1, low(p)], rssem.at[k, PARTS + p])
            for j in range(p, p + 1):
                side[k, 1, 4 + j] = (side[k, 1, 4 + j].astype(F32) + relay[k, 1, j].astype(F32)).astype(BF)
            send(side.at[k, 1, high_of(p)], got.at[k, 1, high_of(p)], ssem, rssem.at[k, 3 * PARTS + p], to_dn)

    def give_back(k, j):
        total = rout[k, j].astype(F32) + got[k, 0, j].astype(F32) + got[k, 1, j].astype(F32)
        rout[k, j] = total.astype(BF)

    def ship(k, j):
        @pl.when(me == j)
        def _():
            pltpu.make_async_copy(rout.at[k, j], ret.at[k, me], retsem.at[k]).start()

        @pl.when(me != j)
        def _():
            send(rout.at[k, j], ret.at[k, me], s_ret.at[k], retsem.at[k], {"expert": j})

    def first_layer_sum_end(k):
        wait_bytes(got.at[k, 1, lo], rssem.at[k, 4 * PARTS + 1])
        wait_bytes(got.at[k, 0, hi], rssem.at[k, 4 * PARTS])
        for p in range(PARTS):
            for which in (0, 1):
                j = 4 * which + p
                wait_bytes(got.at[k, which, pl.ds(j, 1)], rssem.at[k, (2 + which) * PARTS + p])
                give_back(k, j)
                ship(k, j)

    def sum_start(k):
        @pl.when(sec == 0)
        def _():
            first_layer_sum_start(k)

        @pl.when(sec > 0)
        def _():
            spread_start(k)

    def sum_relay(k):
        @pl.when(sec == 0)
        def _():
            first_layer_sum_relay(k)

    def sum_end(k):
        @pl.when(sec == 0)
        def _():
            first_layer_sum_end(k)

        @pl.when(sec > 0)
        def _():
            spread_end(k)

    def publish(k):
        m, half = k // 2, lax.rem(k, 2)
        mine = pl.ds(pl.multiple_of(me * 128, 128), 128)
        for i in range(4):
            owner = half * 4 + i
            block = hnew.at[k, pl.ds(i * 64, 64), :]
            place_at = outbuf.at[m, :, mine]

            @pl.when(owner == me)
            def _():
                pltpu.make_async_copy(block, place_at, osem).start()

            @pl.when(owner != me)
            def _():
                send(block, place_at, s_out.at[k, i], osem, {"expert": owner})

    def home(k):
        @pl.when(sec > 0)
        def _():
            wait_bytes(hin.at[k], hsem.at[k])

        wait_bytes(ret.at[k], retsem.at[k])
        back = ret[k].reshape(640, 128)
        update = jnp.dot(comb[k, 0], back, preferred_element_type=F32)
        update = update + jnp.dot(comb[k, 1], back, preferred_element_type=F32)
        fresh = (hin[k].astype(F32) + update).astype(BF)

        @pl.when(sec < last)
        def _():
            side = 1 + 2 * lax.rem(sec, 2)
            for o in (2, side, 4 - side, 0):
                base = lax.rem(chip + o, 4) * 2
                rows = pl.ds(pl.multiple_of(base * 80, 160), 160)
                moved = jnp.dot(place[k, rows], fresh, preferred_element_type=F32).astype(BF)
                for c in range(2):
                    dout[k, base + c] = moved[c * 80 : (c + 1) * 80]
                    send(
                        dout.at[k, base + c], xs.at[k, 0, my_piece], s_disp.at[k], dsem.at[k, my_piece],
                        {"pipe": sec + 1, "expert": base + c},
                    )

        hnew[k] = fresh

        @pl.when(sec < last)
        def _():
            send(hnew.at[k], hin.at[k], s_h.at[k], hsem.at[k], {"pipe": sec + 1})

        @pl.when(sec == last)
        def _():
            publish(k)

    @pl.when(sec == 0)
    def _():
        def turn(k, carry):
            @pl.when((k < CHUNKS))
            def _():
                gather_start(k)
                prepare(k)

            @pl.when((k >= 1))
            def _():
                sum_end(k - 1)

            @pl.when((k < CHUNKS))
            def _():
                gather_relay(k)
                feed_forward(k)

            @pl.when((k >= 1))
            def _():
                home(k - 1)

            @pl.when((k < CHUNKS))
            def _():
                sum_start(k)
                sum_relay(k)

            return carry

        lax.fori_loop(0, CHUNKS + 1, turn, 0)

    @pl.when(sec > 0)
    def _():
        def turn(k, carry):
            @pl.when((k < CHUNKS))
            def _():
                gather_start(k)
                prepare(k)
                gather_relay(k)

            @pl.when((k >= 1))
            def _():
                home(k - 1)

            @pl.when((k < CHUNKS))
            def _():
                feed_forward(k)
                sum_start(k)
                sum_relay(k)
                sum_end(k)

            return carry

        lax.fori_loop(0, CHUNKS + 1, turn, 0)

    @pl.when(sec < last)
    def _():
        lax.fori_loop(0, CHUNKS, lambda k, carry: (publish(k), carry)[1], 0)

    for o in range(7):
        wait_bytes(table, s_tab.at[o])

    @pl.when(sec > 0)
    def _():
        for e in range(8):
            wait_bytes(table, s_tab.at[7 + e])
        for i in range(4):
            wait_bytes(relay_w.at[0] if i < 2 else wd.at[0], s_dw.at[i])
        for i in range(2):
            wait_bytes(relay_w.at[i], s_dw.at[4 + i])

    @pl.when(sec == 0)
    def _():
        for m in range(2):
            for o in range(7):
                wait_bytes(hin.at[m, pl.ds(0, 64), :], s_tok.at[m, o])
        for k in range(CHUNKS):
            wait_bytes(dfirst.at[k, pl.ds(0, 7)], s_first.at[k])

    def drain(k, carry):
        wait_bytes(xs.at[k, pl.ds(0, 3)], s_ag.at[k])

        @pl.when(sec == 0)
        def _():
            wait_bytes(xs.at[k, pl.ds(0, 3)], s_rs.at[k])

        @pl.when(sec > 0)
        def _():
            wait_bytes(hid.at[k, pl.ds(0, 3)], s_rs.at[k])

        wait_bytes(ret.at[k, pl.ds(0, 7)], s_ret.at[k])

        @pl.when(sec < last)
        def _():
            wait_bytes(dout.at[k], s_disp.at[k])
            wait_bytes(hnew.at[k], s_h.at[k])

        for i in range(4):
            owner = lax.rem(k, 2) * 4 + i

            @pl.when(owner != me)
            def _():
                wait_bytes(hnew.at[k, pl.ds(i * 64, 64), :], s_out.at[k, i])

        return carry

    lax.fori_loop(0, CHUNKS, drain, 0)
    wait_bytes(outbuf, osem)
    final = pltpu.make_async_copy(outbuf, out, wsem.at[0])
    final.start()
    final.wait()


def local(tokens, gains, route_ids, route_weights, picks, w_gate, w_up, w_down):
    vmem = pl.BlockSpec(memory_space=pltpu.VMEM)
    anywhere = pl.BlockSpec(memory_space=pl.ANY)
    dma = pltpu.SemaphoreType.DMA
    out = pl.pallas_call(
        relay_kernel,
        name="relay",
        out_shape=jax.ShapeDtypeStruct((2, 64, 1024), BF),
        in_specs=[anywhere, vmem, vmem, vmem, vmem, anywhere, anywhere, anywhere],
        out_specs=anywhere,
        scratch_shapes=[
            pltpu.VMEM((4, 1024, 768), BF),
            pltpu.VMEM((4, 384, 1024), BF),
            pltpu.VMEM((8, 256), F32),
            pltpu.VMEM((2, 8, 8, 256), F32),
            pltpu.VMEM((CHUNKS, 640, 256), BF),
            pltpu.VMEM((CHUNKS, 2, 256, 640), BF),
            pltpu.VMEM((CHUNKS, 256, 128), BF),
            pltpu.VMEM((CHUNKS, 256, 128), BF),
            pltpu.VMEM((CHUNKS, 4, 8, 80, 128), BF),
            pltpu.VMEM((CHUNKS, 8, 80, 128), BF),
            pltpu.VMEM((CHUNKS, 8, 80, 128), BF),
            pltpu.VMEM((80, 768), F32),
            pltpu.VMEM((80, 128), F32),
            pltpu.VMEM((CHUNKS, 4, 80, 384), BF),
            pltpu.VMEM((80, 1024), F32),
            pltpu.VMEM((2, 192, 1024), BF),
            pltpu.VMEM((CHUNKS, 8, 80, 128), BF),
            pltpu.VMEM((CHUNKS, 2, 8, 80, 128), BF),
            pltpu.VMEM((CHUNKS, 2, 4, 80, 128), BF),
            pltpu.VMEM((CHUNKS, 2, 8, 80, 128), BF),
            pltpu.VMEM((CHUNKS, 8, 80, 128), BF),
            pltpu.VMEM((CHUNKS, 8, 80, 128), BF),
            pltpu.VMEM((2, 64, 1024), BF),
            dma((12,)),
            dma((6,)),
            dma((2,)),
            dma((CHUNKS,)),
            dma((CHUNKS, 2 * PARTS)),
            dma((CHUNKS, 4 * PARTS + 2)),
            dma((CHUNKS, 4 * PARTS + 2)),
            dma((CHUNKS,)),
            dma(()),
            dma((15,)),
            dma((6,)),
            dma((2, 7)),
            dma((CHUNKS,)),
            dma((CHUNKS,)),
            dma((CHUNKS,)),
            dma((CHUNKS,)),
            dma((CHUNKS,)),
            dma((CHUNKS,)),
            dma((CHUNKS, 4)),
        ],
        compiler_params=pltpu.CompilerParams(
            collective_id=0, has_side_effects=True, vmem_limit_bytes=56 * 1024 * 1024
        ),
    )(
        tokens, gains, jnp.swapaxes(route_ids[0], 1, 2), jnp.swapaxes(route_weights[0], 1, 2),
        picks[0, :, 0], w_gate[0, 0], w_up[0, 0], w_down[0, 0],
    )
    return out[None]


def solution(mesh):
    return jax.shard_map(
        local,
        mesh=mesh,
        in_specs=(
            P(None, "expert", None),
            P("pipe", None),
            P("pipe", None, "expert", None),
            P("pipe", None, "expert", None),
            P("pipe", None, "expert", None),
            P("pipe", "expert", None, "tensor"),
            P("pipe", "expert", None, "tensor"),
            P("pipe", "expert", "tensor", None),
        ),
        out_specs=P("pipe", None, "expert", "tensor"),
        check_vma=False,
    )
```

```python
import jax
import jax.numpy as jnp
from jax import lax
from jax.experimental import pallas as pl
from jax.experimental.pallas import tpu as pltpu
from jax.sharding import PartitionSpec as P

EPS = 1e-06
MESH = pl.DeviceIdType.MESH
BF = jnp.bfloat16
F32 = jnp.float32
CHUNKS = 4
CAP = 5
PARTS = 4


def wait_bytes(ref, sem):
    pltpu.make_async_copy(ref, ref, sem).wait()


def relay_kernel(
    tokens, gains, ids, route_w, picks, w_gate, w_up, w_down, out,
    wgu, wd, table, tables, place, comb, hin, hnew, xs, dfirst, dout, acc, squares, hid, total, relay_w,
    opp, side, relay, got, rout, ret, outbuf,
    wsem, dwsem, tsem, hsem, dsem, agsem, rssem, retsem, osem,
    s_tab, s_dw, s_tok, s_first, s_disp, s_ag, s_rs, s_ret, s_h, s_out,
):
    sec = lax.axis_index("pipe")
    rank = lax.axis_index("tensor")
    me = lax.axis_index("expert")
    last = lax.axis_size("pipe") - 1
    up1 = lax.rem(rank + 1, 4)
    dn1 = lax.rem(rank + 3, 4)
    far = lax.rem(rank + 2, 4)
    my_half = me // 4
    chip, core = me // 2, lax.rem(me, 2)
    partner = chip * 2 + 1 - core
    my_piece = core * 4 + chip

    def send(src, dst, ssem, rsem, dev):
        pltpu.make_async_remote_copy(
            src_ref=src, dst_ref=dst, send_sem=ssem, recv_sem=rsem,
            device_id=dev, device_id_type=MESH,
        ).start()

    barrier = pltpu.get_barrier_semaphore()

    def greet(dev):
        pl.semaphore_signal(barrier, inc=1, device_id=dev, device_id_type=MESH)

    for o in range(1, 8):
        greet({"expert": lax.rem(me + o, 8)})
    greet({"tensor": up1})
    greet({"tensor": dn1})
    greet({"tensor": far})

    @pl.when(sec < last)
    def _():
        for e in range(8):
            greet({"pipe": sec + 1, "expert": e})

    @pl.when(sec > 0)
    def _():
        for e in range(8):
            greet({"pipe": sec - 1, "expert": e})

    def weight_copies():
        copies = []
        for q in range(4):
            copies.append((w_gate.at[pl.ds(q * 1024, 1024), :], wgu.at[q, :, pl.ds(0, 384)]))
            copies.append((w_up.at[pl.ds(q * 1024, 1024), :], wgu.at[q, :, pl.ds(384, 384)]))
        return [pltpu.make_async_copy(a, b, wsem.at[i]) for i, (a, b) in enumerate(copies)]

    def slice_of_down(q):
        return w_down.at[:, pl.ds(pl.multiple_of(q * 1024, 128), 1024)]

    def first_down_copies():
        return [pltpu.make_async_copy(slice_of_down(q), wd.at[q], wsem.at[8 + q]) for q in range(4)]

    def own_down_copy():
        return pltpu.make_async_copy(slice_of_down(rank), wd.at[rank], wsem.at[8])

    for copy in weight_copies():
        copy.start()

    @pl.when(sec == 0)
    def _():
        for copy in first_down_copies():
            copy.start()

    @pl.when(sec > 0)
    def _():
        own_down_copy().start()

    def iota(shape, dim):
        return lax.broadcasted_iota(jnp.int32, shape, dim).astype(F32)

    def column(row, eye):
        return jnp.sum(jnp.where(eye, row, 0.0), axis=1, keepdims=True)

    sub, lane = iota((64, 64), 0), iota((64, 64), 1)
    eye = sub == lane
    shift = (lax.rem(me, 4) * 64).astype(F32)
    spread = (iota((64, 256), 0) + shift) == iota((64, 256), 1)
    row_of = iota((8, 256), 0)
    whole = jnp.zeros((8, 256), F32)
    for m in range(2):
        picked = column(picks[m : m + 1, :].astype(F32), eye)
        spot = jnp.sum(jnp.where(picked == lane, sub, 0.0), axis=0, keepdims=True)
        spot_col = column(spot, eye)
        quarter, quarter_col = jnp.floor(spot / 16.0), jnp.floor(spot_col / 16.0)
        names = [ids[m, t : t + 1, :].astype(F32) for t in range(2)]
        name_cols = [column(n, eye) for n in names]
        for t in range(2):
            slot = jnp.zeros((1, 64), F32)
            for u in range(2):
                hit = (name_cols[u] == names[t]) & (quarter_col == quarter)
                hit = hit & (spot_col * 2.0 + u < spot * 2.0 + t)
                slot = slot + jnp.sum(jnp.where(hit, 1.0, 0.0), axis=0, keepdims=True)
            at = names[t] * 80.0 + lax.rem(me, 4).astype(F32) * 20.0 + quarter * CAP + slot
            at = jnp.where(slot < CAP, at, -1.0)
            for field, value in ((t, at), (2 + t, route_w[m, t : t + 1, :])):
                placed = jnp.where(spread, column(value, eye), 0.0)
                placed = jnp.sum(placed, axis=0, keepdims=True)
                whole = whole + jnp.where(row_of == m * 4 + field, placed, 0.0)
    table[...] = whole

    greeted = 10 + jnp.where(sec < last, 8, 0) + jnp.where(sec > 0, 8, 0)
    pl.semaphore_wait(barrier, greeted)

    for o in range(1, 8):
        send(table, tables.at[0, me], s_tab.at[o - 1], tsem.at[0], {"expert": lax.rem(me + o, 8)})
    pltpu.make_async_copy(table, tables.at[0, me], tsem.at[0]).start()

    @pl.when(sec > 0)
    def _():
        for e in range(8):
            send(table, tables.at[1, me], s_tab.at[7 + e], tsem.at[1], {"pipe": sec - 1, "expert": e})

    @pl.when(sec == 0)
    def _():
        start = pl.multiple_of(rank * 1024, 128)
        row = pl.multiple_of(lax.rem(me, 4) * 64, 64)
        for m in range(2):
            k = m * 2 + my_half
            for o in range(1, 8):
                j = lax.rem(me + o, 8)
                send(
                    tokens.at[m, :, pl.ds(pl.multiple_of(start + j * 128, 128), 128)],
                    hin.at[k, pl.ds(row, 64), :],
                    s_tok.at[m, o - 1], hsem.at[k], {"expert": j},
                )
            pltpu.make_async_copy(
                tokens.at[m, :, pl.ds(pl.multiple_of(start + me * 128, 128), 128)],
                hin.at[k, pl.ds(row, 64), :], hsem.at[k],
            ).start()

    to_up, to_dn = {"tensor": up1}, {"tensor": dn1}
    top, rest = pl.ds(0, 192), pl.ds(192, 192)

    @pl.when(sec > 0)
    def _():
        distant = pl.ds(pl.multiple_of(far * 1024, 128), 1024)
        send(w_down.at[top, distant], relay_w.at[0], s_dw.at[0], dwsem.at[2], to_up)
        send(w_down.at[rest, distant], relay_w.at[1], s_dw.at[1], dwsem.at[3], to_dn)
        send(slice_of_down(up1), wd.at[rank], s_dw.at[2], dwsem.at[0], to_up)
        send(slice_of_down(dn1), wd.at[rank], s_dw.at[3], dwsem.at[1], to_dn)
        wait_bytes(relay_w.at[0], dwsem.at[2])
        send(relay_w.at[0], wd.at[dn1, top], s_dw.at[4], dwsem.at[4], to_up)
        wait_bytes(relay_w.at[1], dwsem.at[3])
        send(relay_w.at[1], wd.at[up1, rest], s_dw.at[5], dwsem.at[5], to_dn)

    slot_rows = iota((640, 256), 0)
    slot_cols = iota((256, 640), 1)
    eye256 = iota((256, 256), 0) == iota((256, 256), 1)

    def fields(which, k, names):
        m, half = k // 2, lax.rem(k, 2)
        rows = []
        for f in names:
            at = pl.ds(m * 4 + f, 1)
            row = tables[which, half * 4, at, :]
            for i in range(1, 4):
                row = row + tables[which, half * 4 + i, at, :]
            rows.append(row)
        return rows

    def placing(which, k):
        a, b = fields(which, k, (0, 1))
        return jnp.where((slot_rows == a) | (slot_rows == b), 1.0, 0.0).astype(BF)

    def place_rows(matrix, rows, dest, k):
        moved = jnp.dot(matrix, rows, preferred_element_type=F32).astype(BF)
        for e in range(8):
            dest[k, e] = moved[e * 80 : (e + 1) * 80]

    def far_first(side):
        order = [lax.rem(chip + o, 4) * 2 for o in (2, side, 4 - side)]
        return [base + c for base in order for c in range(2)]

    def first(k):
        place_rows(placing(0, k), hin[k], dfirst, k)
        for o in range(1, 8):
            e = lax.rem(me + o, 8)
            send(dfirst.at[k, e], xs.at[k, 0, my_piece], s_first.at[k], dsem.at[k, my_piece], {"expert": e})
        pltpu.make_async_copy(dfirst.at[k, me], xs.at[k, 0, my_piece], dsem.at[k, my_piece]).start()

    @pl.when(sec == 0)
    def _():
        wait_bytes(tables.at[0], tsem.at[0])
        wait_bytes(hin.at[0], hsem.at[0])
        first(0)

    def prepare(k):
        @pl.when((k < CHUNKS - 1) & (sec == 0))
        def _():
            wait_bytes(hin.at[k + 1], hsem.at[k + 1])
            first(k + 1)

        @pl.when((k == 0) & (sec > 0))
        def _():
            wait_bytes(tables.at[0], tsem.at[0])

        @pl.when((k == 0) & (sec < last))
        def _():
            wait_bytes(tables.at[1], tsem.at[1])

        cols = [column(row, eye256) for row in fields(0, k, (0, 1, 2, 3))]
        mix = jnp.where(slot_cols == cols[0], cols[2], 0.0)
        mix = mix + jnp.where(slot_cols == cols[1], cols[3], 0.0)
        high = mix.astype(BF)
        comb[k, 0] = high
        comb[k, 1] = (mix - high.astype(F32)).astype(BF)

        @pl.when(sec < last)
        def _():
            place[k] = placing(1, k)

        @pl.when(k == 0)
        def _():
            for copy in weight_copies():
                copy.wait()

        @pl.when((k == 0) & (sec == 0))
        def _():
            for copy in first_down_copies():
                copy.wait()

        @pl.when((k == 0) & (sec > 0))
        def _():
            own_down_copy().wait()
            wait_bytes(wd.at[dn1], dwsem.at[0])
            wait_bytes(wd.at[up1], dwsem.at[1])
            wait_bytes(wd.at[far, top], dwsem.at[4])
            wait_bytes(wd.at[far, rest], dwsem.at[5])

    lo, hi = pl.ds(0, 4), pl.ds(4, 4)

    def lanes(value, j):
        return value[:, j * 128 : (j + 1) * 128]

    def part(k, rel, origin):
        x = jnp.concatenate([xs[k, rel, (j % 2) * 4 + j // 2] for j in range(8)], axis=1).astype(F32)
        scaled = x * gains[:, pl.ds(pl.multiple_of(origin * 1024, 128), 1024)]
        both = jnp.dot(scaled.astype(BF), wgu[origin], preferred_element_type=F32)
        return jnp.sum(x * x, axis=1, keepdims=True), both

    def chips():
        return [lax.rem(chip + o, 4) for o in (0, 1, 3, 2)]

    def low(p):
        return pl.ds(p, 1)

    def high_of(p):
        return pl.ds(4 + p, 1)

    def gather_start(k):
        ssem = s_ag.at[k]
        for p in chips():
            wait_bytes(xs.at[k, 0, low(p)], dsem.at[k, p])
            send(xs.at[k, 0, low(p)], xs.at[k, 1, low(p)], ssem, agsem.at[k, p], to_up)
            wait_bytes(xs.at[k, 0, high_of(p)], dsem.at[k, PARTS + p])
            send(xs.at[k, 0, high_of(p)], xs.at[k, 2, high_of(p)], ssem, agsem.at[k, PARTS + p], to_dn)
        send(xs.at[k, 0, lo], xs.at[k, 2, lo], ssem, agsem.at[k, 4 * PARTS], to_dn)
        send(xs.at[k, 0, hi], xs.at[k, 1, hi], ssem, agsem.at[k, 4 * PARTS + 1], to_up)

    def gather_relay(k):
        ssem = s_ag.at[k]
        sq, both = part(k, 0, rank)
        acc[...] = both
        squares[...] = jnp.broadcast_to(sq, (80, 128))
        for p in chips():
            wait_bytes(xs.at[k, 1, low(p)], agsem.at[k, p])
            send(xs.at[k, 1, low(p)], xs.at[k, 3, low(p)], ssem, agsem.at[k, 2 * PARTS + p], to_up)
            wait_bytes(xs.at[k, 2, high_of(p)], agsem.at[k, PARTS + p])
            send(xs.at[k, 2, high_of(p)], xs.at[k, 3, high_of(p)], ssem, agsem.at[k, 3 * PARTS + p], to_dn)

    def feed_forward(k):
        both, sq = acc[...], squares[:, 0:1]
        wait_bytes(xs.at[k, 1, hi], agsem.at[k, 4 * PARTS + 1])
        s, b = part(k, 1, dn1)
        sq, both = sq + s, both + b
        wait_bytes(xs.at[k, 2, lo], agsem.at[k, 4 * PARTS])
        s, b = part(k, 2, up1)
        sq, both = sq + s, both + b
        for p in range(PARTS):
            wait_bytes(xs.at[k, 3, low(p)], agsem.at[k, 2 * PARTS + p])
            wait_bytes(xs.at[k, 3, high_of(p)], agsem.at[k, 3 * PARTS + p])
        s, b = part(k, 3, far)
        sq, both = sq + s, both + b
        both = both * lax.rsqrt(sq * (1.0 / 4096.0) + EPS)
        gate, up = both[:, :384], both[:, 384:]
        hid[k, 0] = (gate / (1.0 + jnp.exp(-gate)) * up).astype(BF)

    def down(k, q):
        return jnp.dot(hid[k, 0], wd[q], preferred_element_type=F32).astype(BF)

    def spread_start(k):
        ssem = s_rs.at[k]
        send(hid.at[k, 0], hid.at[k, 1], ssem, rssem.at[k, 0], to_up)
        send(hid.at[k, 0], hid.at[k, 2], ssem, rssem.at[k, 1], to_dn)
        send(hid.at[k, 0], hid.at[k, 3], ssem, rssem.at[k, 2], {"tensor": far})
        total[...] = jnp.dot(hid[k, 0], wd[rank], preferred_element_type=F32)

    def spread_end(k):
        wait_bytes(hid.at[k, 1], rssem.at[k, 0])
        total[...] += jnp.dot(hid[k, 1], wd[dn1], preferred_element_type=F32)
        wait_bytes(hid.at[k, 2], rssem.at[k, 1])
        total[...] += jnp.dot(hid[k, 2], wd[up1], preferred_element_type=F32)
        wait_bytes(hid.at[k, 3], rssem.at[k, 2])
        done = (total[...] + jnp.dot(hid[k, 3], wd[far], preferred_element_type=F32)).astype(BF)
        for j in range(8):
            rout[k, j] = lanes(done, j)
        for j in far_first(1):
            send(rout.at[k, j], ret.at[k, me], s_ret.at[k], retsem.at[k], {"expert": j})
        send(rout.at[k, partner], ret.at[k, me], s_ret.at[k], retsem.at[k], {"expert": partner})
        pltpu.make_async_copy(rout.at[k, me], ret.at[k, me], retsem.at[k]).start()

    def first_layer_sum_start(k):
        ssem = s_rs.at[k]
        value = down(k, far)
        for j in range(8):
            opp[k, j] = lanes(value, j)
        for p in range(PARTS):
            send(opp.at[k, low(p)], relay.at[k, 0, low(p)], ssem, rssem.at[k, p], to_up)
            send(opp.at[k, high_of(p)], relay.at[k, 1, low(p)], ssem, rssem.at[k, PARTS + p], to_dn)
        value = down(k, up1)
        for j in range(8):
            side[k, 0, j] = lanes(value, j)
        send(side.at[k, 0, hi], got.at[k, 0, hi], ssem, rssem.at[k, 4 * PARTS], to_up)
        value = down(k, dn1)
        for j in range(8):
            side[k, 1, j] = lanes(value, j)
        send(side.at[k, 1, lo], got.at[k, 1, lo], ssem, rssem.at[k, 4 * PARTS + 1], to_dn)
        value = down(k, rank)
        for j in range(8):
            rout[k, j] = lanes(value, j)

    def first_layer_sum_relay(k):
        ssem = s_rs.at[k]
        for p in range(PARTS):
            wait_bytes(relay.at[k, 0, low(p)], rssem.at[k, p])
            for j in range(p, p + 1):
                side[k, 0, j] = (side[k, 0, j].astype(F32) + relay[k, 0, j].astype(F32)).astype(BF)
            send(side.at[k, 0, low(p)], got.at[k, 0, low(p)], ssem, rssem.at[k, 2 * PARTS + p], to_up)
            wait_bytes(relay.at[k, 1, low(p)], rssem.at[k, PARTS + p])
            for j in range(p, p + 1):
                side[k, 1, 4 + j] = (side[k, 1, 4 + j].astype(F32) + relay[k, 1, j].astype(F32)).astype(BF)
            send(side.at[k, 1, high_of(p)], got.at[k, 1, high_of(p)], ssem, rssem.at[k, 3 * PARTS + p], to_dn)

    def give_back(k, j):
        total = rout[k, j].astype(F32) + got[k, 0, j].astype(F32) + got[k, 1, j].astype(F32)
        rout[k, j] = total.astype(BF)

    def ship(k, j):
        @pl.when(me == j)
        def _():
            pltpu.make_async_copy(rout.at[k, j], ret.at[k, me], retsem.at[k]).start()

        @pl.when(me != j)
        def _():
            send(rout.at[k, j], ret.at[k, me], s_ret.at[k], retsem.at[k], {"expert": j})

    def first_layer_sum_end(k):
        wait_bytes(got.at[k, 1, lo], rssem.at[k, 4 * PARTS + 1])
        wait_bytes(got.at[k, 0, hi], rssem.at[k, 4 * PARTS])
        for p in range(PARTS):
            for which in (0, 1):
                j = 4 * which + p
                wait_bytes(got.at[k, which, pl.ds(j, 1)], rssem.at[k, (2 + which) * PARTS + p])
                give_back(k, j)
                ship(k, j)

    def sum_start(k):
        @pl.when(sec == 0)
        def _():
            first_layer_sum_start(k)

        @pl.when(sec > 0)
        def _():
            spread_start(k)

    def sum_relay(k):
        @pl.when(sec == 0)
        def _():
            first_layer_sum_relay(k)

    def sum_end(k):
        @pl.when(sec == 0)
        def _():
            first_layer_sum_end(k)

        @pl.when(sec > 0)
        def _():
            spread_end(k)

    def publish(k):
        m, half = k // 2, lax.rem(k, 2)
        mine = pl.ds(pl.multiple_of(me * 128, 128), 128)
        for i in range(4):
            owner = half * 4 + i
            block = hnew.at[k, pl.ds(i * 64, 64), :]
            place_at = outbuf.at[m, :, mine]

            @pl.when(owner == me)
            def _():
                pltpu.make_async_copy(block, place_at, osem).start()

            @pl.when(owner != me)
            def _():
                send(block, place_at, s_out.at[k, i], osem, {"expert": owner})

    def home(k):
        @pl.when(sec > 0)
        def _():
            wait_bytes(hin.at[k], hsem.at[k])

        wait_bytes(ret.at[k], retsem.at[k])
        back = ret[k].reshape(640, 128)
        update = jnp.dot(comb[k, 0], back, preferred_element_type=F32)
        update = update + jnp.dot(comb[k, 1], back, preferred_element_type=F32)
        fresh = (hin[k].astype(F32) + update).astype(BF)

        @pl.when(sec < last)
        def _():
            place_rows(place[k], fresh, dout, k)
            for e in far_first(1 + 2 * lax.rem(sec, 2)) + [chip * 2, chip * 2 + 1]:
                send(
                    dout.at[k, e], xs.at[k, 0, my_piece], s_disp.at[k], dsem.at[k, my_piece],
                    {"pipe": sec + 1, "expert": e},
                )

        hnew[k] = fresh

        @pl.when(sec < last)
        def _():
            send(hnew.at[k], hin.at[k], s_h.at[k], hsem.at[k], {"pipe": sec + 1})

        @pl.when(sec == last)
        def _():
            publish(k)

    @pl.when(sec == 0)
    def _():
        def turn(k, carry):
            @pl.when((k < CHUNKS))
            def _():
                gather_start(k)
                prepare(k)

            @pl.when((k >= 1))
            def _():
                sum_end(k - 1)

            @pl.when((k < CHUNKS))
            def _():
                gather_relay(k)
                feed_forward(k)

            @pl.when((k >= 1))
            def _():
                home(k - 1)

            @pl.when((k < CHUNKS))
            def _():
                sum_start(k)
                sum_relay(k)

            return carry

        lax.fori_loop(0, CHUNKS + 1, turn, 0)

    @pl.when(sec > 0)
    def _():
        def turn(k, carry):
            @pl.when((k < CHUNKS))
            def _():
                gather_start(k)
                prepare(k)
                gather_relay(k)

            @pl.when((k >= 1))
            def _():
                home(k - 1)

            @pl.when((k < CHUNKS))
            def _():
                feed_forward(k)
                sum_start(k)
                sum_relay(k)
                sum_end(k)

            return carry

        lax.fori_loop(0, CHUNKS + 1, turn, 0)

    @pl.when(sec < last)
    def _():
        lax.fori_loop(0, CHUNKS, lambda k, carry: (publish(k), carry)[1], 0)

    for o in range(7):
        wait_bytes(table, s_tab.at[o])

    @pl.when(sec > 0)
    def _():
        for e in range(8):
            wait_bytes(table, s_tab.at[7 + e])
        for i in range(4):
            wait_bytes(relay_w.at[0] if i < 2 else wd.at[0], s_dw.at[i])
        for i in range(2):
            wait_bytes(relay_w.at[i], s_dw.at[4 + i])

    @pl.when(sec == 0)
    def _():
        for m in range(2):
            for o in range(7):
                wait_bytes(hin.at[m, pl.ds(0, 64), :], s_tok.at[m, o])
        for k in range(CHUNKS):
            wait_bytes(dfirst.at[k, pl.ds(0, 7)], s_first.at[k])

    def drain(k, carry):
        wait_bytes(xs.at[k, pl.ds(0, 3)], s_ag.at[k])

        @pl.when(sec == 0)
        def _():
            wait_bytes(xs.at[k, pl.ds(0, 3)], s_rs.at[k])

        @pl.when(sec > 0)
        def _():
            wait_bytes(hid.at[k, pl.ds(0, 3)], s_rs.at[k])

        wait_bytes(ret.at[k, pl.ds(0, 7)], s_ret.at[k])

        @pl.when(sec < last)
        def _():
            wait_bytes(dout.at[k], s_disp.at[k])
            wait_bytes(hnew.at[k], s_h.at[k])

        for i in range(4):
            owner = lax.rem(k, 2) * 4 + i

            @pl.when(owner != me)
            def _():
                wait_bytes(hnew.at[k, pl.ds(i * 64, 64), :], s_out.at[k, i])

        return carry

    lax.fori_loop(0, CHUNKS, drain, 0)
    wait_bytes(outbuf, osem)
    final = pltpu.make_async_copy(outbuf, out, wsem.at[0])
    final.start()
    final.wait()


def local(tokens, gains, route_ids, route_weights, picks, w_gate, w_up, w_down):
    vmem = pl.BlockSpec(memory_space=pltpu.VMEM)
    anywhere = pl.BlockSpec(memory_space=pl.ANY)
    dma = pltpu.SemaphoreType.DMA
    out = pl.pallas_call(
        relay_kernel,
        name="relay",
        out_shape=jax.ShapeDtypeStruct((2, 64, 1024), BF),
        in_specs=[anywhere, vmem, vmem, vmem, vmem, anywhere, anywhere, anywhere],
        out_specs=anywhere,
        scratch_shapes=[
            pltpu.VMEM((4, 1024, 768), BF),
            pltpu.VMEM((4, 384, 1024), BF),
            pltpu.VMEM((8, 256), F32),
            pltpu.VMEM((2, 8, 8, 256), F32),
            pltpu.VMEM((CHUNKS, 640, 256), BF),
            pltpu.VMEM((CHUNKS, 2, 256, 640), BF),
            pltpu.VMEM((CHUNKS, 256, 128), BF),
            pltpu.VMEM((CHUNKS, 256, 128), BF),
            pltpu.VMEM((CHUNKS, 4, 8, 80, 128), BF),
            pltpu.VMEM((CHUNKS, 8, 80, 128), BF),
            pltpu.VMEM((CHUNKS, 8, 80, 128), BF),
            pltpu.VMEM((80, 768), F32),
            pltpu.VMEM((80, 128), F32),
            pltpu.VMEM((CHUNKS, 4, 80, 384), BF),
            pltpu.VMEM((80, 1024), F32),
            pltpu.VMEM((2, 192, 1024), BF),
            pltpu.VMEM((CHUNKS, 8, 80, 128), BF),
            pltpu.VMEM((CHUNKS, 2, 8, 80, 128), BF),
            pltpu.VMEM((CHUNKS, 2, 4, 80, 128), BF),
            pltpu.VMEM((CHUNKS, 2, 8, 80, 128), BF),
            pltpu.VMEM((CHUNKS, 8, 80, 128), BF),
            pltpu.VMEM((CHUNKS, 8, 80, 128), BF),
            pltpu.VMEM((2, 64, 1024), BF),
            dma((12,)),
            dma((6,)),
            dma((2,)),
            dma((CHUNKS,)),
            dma((CHUNKS, 2 * PARTS)),
            dma((CHUNKS, 4 * PARTS + 2)),
            dma((CHUNKS, 4 * PARTS + 2)),
            dma((CHUNKS,)),
            dma(()),
            dma((15,)),
            dma((6,)),
            dma((2, 7)),
            dma((CHUNKS,)),
            dma((CHUNKS,)),
            dma((CHUNKS,)),
            dma((CHUNKS,)),
            dma((CHUNKS,)),
            dma((CHUNKS,)),
            dma((CHUNKS, 4)),
        ],
        compiler_params=pltpu.CompilerParams(
            collective_id=0, has_side_effects=True, vmem_limit_bytes=56 * 1024 * 1024
        ),
    )(
        tokens, gains, jnp.swapaxes(route_ids[0], 1, 2), jnp.swapaxes(route_weights[0], 1, 2),
        picks[0, :, 0], w_gate[0, 0], w_up[0, 0], w_down[0, 0],
    )
    return out[None]


def solution(mesh):
    return jax.shard_map(
        local,
        mesh=mesh,
        in_specs=(
            P(None, "expert", None),
            P("pipe", None),
            P("pipe", None, "expert", None),
            P("pipe", None, "expert", None),
            P("pipe", None, "expert", None),
            P("pipe", "expert", None, "tensor"),
            P("pipe", "expert", None, "tensor"),
            P("pipe", "expert", "tensor", None),
        ),
        out_specs=P("pipe", None, "expert", "tensor"),
        check_vma=False,
    )
```
